256 devices in a mesh: dp: 256 (over y, x, z, core).
Axes of the slice: x: 4, y: 4, z: 8, core: 2. Of those that a mesh axis runs over, the one named last changes fastest.
Arguments:
- image_emb: bfloat16 [2048, 1152], P('dp'), may hold values from -0.4375 to 0.4375
- text_tokens: bfloat16 [65536, 1152], P('dp'), may hold values from -0.078125 to 0.078125
- caption_ids: int32 [65536], P('dp'), may hold values from 0 to 2047, as said below
- groups: int32 [2048], P('dp'), may hold values from 0 to 511
- text_gain: float32 [1152], replicated, may hold values from 0.5 to 1.5
- log_scale: float32 [1], replicated, may hold values from 2 to 3
- logit_bias: float32 [1], replicated, may hold values from -3 to -1
Outputs:
- image_grad: float32 [2048, 1152], P('dp')
- token_grad: float32 [65536, 1152], P('dp')
- gain_grad: float32 [1152], replicated
- scalars: float32 [3], replicated
The draws below stay inside these ranges and needn't reach their ends.
Inputs may be any that keep to these rules, and one draw needn't show every extreme that they name: `caption_ids`: caption ids never fall along the rows and every caption 0 .. 2047 has at least one row; the captions of the pairs of device d (ids 8 d to 8 (d + 1) - 1) all begin within the 256 rows of device d; the rows of device d before its first caption all belong to the last caption of device d - 1; device 0 begins with caption 0. `groups`: group ids of the pairs; equal ids mark matching pairs.
All inputs are finite; a program needn't handle non-finite values.
Results may differ from the reference program's by a relative error of at most 0.005.
Values may be sent and summed in bfloat16 or wider, within the bound.
No kernel may reach another device: no remote copies, remote signals or barrier semaphores. Data moves between devices by JAX's collectives and lax.ppermute only.
A program may use at most 64 MiB of HBM per device.

```python
import jax
import jax.numpy as jnp
from jax import lax

D = 1152
PAIRS_DEV = 8
SPILL = 16
TOK_DEV = 256
PAIRS = 2048
TOKENS = 65536
GROUPS = 512
N_DP = 256


def draw_caption_ids(key, part):
    devices = TOKENS // TOK_DEV
    shift_key, weight_key = jax.random.split(jax.random.fold_in(key, 17))
    shifts = jax.random.randint(shift_key, (devices,), 0, SPILL)
    shifts = jnp.where(jnp.arange(devices) == 0, 0, shifts)
    weights = jax.random.randint(weight_key, (devices, PAIRS_DEV), 1, 5)
    cumulative = jnp.cumsum(weights, axis=1)
    extra = TOK_DEV - shifts - PAIRS_DEV
    ends = jnp.arange(1, PAIRS_DEV + 1)[None, :] + extra[:, None] * cumulative // cumulative[:, -1:]
    starts = jnp.concatenate([jnp.zeros((devices, 1), ends.dtype), ends[:, :-1]], axis=1)
    starts = starts + shifts[:, None] + (jnp.arange(devices) * TOK_DEV)[:, None]
    positions = jnp.arange(TOKENS)
    found = jnp.searchsorted(starts.reshape(-1), positions, side='right') - 1
    return found.astype(jnp.int32)


def plant(entries, key, least, high):
    longest = entries.shape.index(max(entries.shape))
    spots = []
    for shift in (0, 1):
        where = [jax.random.randint(jax.random.fold_in(key, axis), (), 0, length) for axis, length in enumerate(entries.shape)]
        where[longest] = (where[longest] + shift) % entries.shape[longest]
        spots.append(tuple(where))
    return entries.at[spots[0]].set(least).at[spots[1]].set(high)


def steps_of(rng, dims, cuts, low, largest):
    gain, own = 1.0, jax.random.fold_in(rng, 6)
    for dim, blocks in cuts:
        heights = jnp.exp(jax.random.uniform(jax.random.fold_in(own, dim), (blocks,), jnp.float32, low / len(cuts), largest / len(cuts)))
        gain = gain * jnp.repeat(heights, dims[dim] // blocks).reshape([-1 if axis == dim else 1 for axis in range(len(dims))])
    return gain


def gaussian(key, dims, deviation, reach, cuts=(), kind=jnp.bfloat16):
    array = deviation * jax.random.normal(key, dims, jnp.float32)
    if cuts:
        array = array * steps_of(key, dims, cuts, -0.22, 0.18)
    return jnp.clip(array, -reach, reach).astype(kind)


def setup_inputs(seed: int = 0) -> dict:
    streams_of = jax.random.split(jax.random.key(seed), 8)
    image_emb = gaussian(streams_of[0], (PAIRS, D), 0.03, 0.4375, ((0, 256),))
    text_tokens = gaussian(streams_of[1], (TOKENS, D), 0.005, 0.078125, ((0, 256),))
    caption_ids = draw_caption_ids(jax.random.fold_in(streams_of[7], 71), 0)
    groups = plant(jax.random.randint(streams_of[3], (PAIRS,), 0, GROUPS), jax.random.fold_in(streams_of[3], 1), 0, GROUPS - 1).astype(jnp.int32)
    text_gain = jnp.clip(1.0 + 0.1 * jax.random.normal(streams_of[4], (D,), jnp.float32), 0.5, 1.5)
    log_scale = jnp.clip(jax.random.uniform(streams_of[5], (1,), jnp.float32, 2.0, 3.0), 2.0, 3.0)
    logit_bias = jnp.clip(jax.random.uniform(streams_of[6], (1,), jnp.float32, -3.0, -1.0), -3.0, -1.0)
    return dict(image_emb=image_emb, text_tokens=text_tokens, caption_ids=caption_ids, groups=groups, text_gain=text_gain, log_scale=log_scale, logit_bias=logit_bias)


def unit_rows(values):
    length = jnp.sqrt(lax.optimization_barrier(jnp.sum(values * values, axis=1, keepdims=True)))
    return (values / length, length)

def reference(image_emb, text_tokens, caption_ids, groups, text_gain, log_scale, logit_bias):
    raw_image = image_emb.astype(jnp.float32)
    unit_image, image_norm = unit_rows(raw_image)
    image_low = unit_image.astype(jnp.bfloat16)
    token_blocks = text_tokens.reshape(N_DP, TOK_DEV, D)
    id_blocks = caption_ids.reshape(N_DP, TOK_DEV)

    def pool_step(pooled, inputs):
        rows_in, ids_in = inputs
        return (pooled + jax.ops.segment_sum(rows_in.astype(jnp.float32), ids_in, num_segments=PAIRS), None)
    pooled, unused = lax.scan(pool_step, jnp.zeros((PAIRS, D), jnp.float32), (token_blocks, id_blocks))
    embedded = pooled * text_gain[None, :]
    unit_text, text_norm = unit_rows(embedded)
    text_low = unit_text.astype(jnp.bfloat16)
    scale_value = jnp.exp(log_scale[0])
    bias_value = logit_bias[0]

    def pair_step(text_total, inputs):
        rows_in, groups_in = inputs
        scaled = scale_value * jnp.dot(rows_in, text_low.T, preferred_element_type=jnp.float32)
        logits = scaled + bias_value
        labels = jnp.where(groups_in[:, None] == groups[None, :], 1.0, -1.0).astype(jnp.float32)
        margin = -labels * logits
        coeffs = -labels * jax.nn.sigmoid(margin)
        coeff_low = coeffs.astype(jnp.bfloat16)
        image_part = scale_value * jnp.dot(coeff_low, text_low, preferred_element_type=jnp.float32)
        text_total = text_total + jnp.dot(coeff_low.T, rows_in, preferred_element_type=jnp.float32)
        sum_terms = jnp.stack([jnp.sum(jax.nn.softplus(margin)), jnp.sum(coeffs * scaled), jnp.sum(coeffs)])
        return (text_total, (image_part, sum_terms))
    text_acc, (image_parts, term_blocks) = lax.scan(pair_step, jnp.zeros((PAIRS, D), jnp.float32), (image_low.reshape(N_DP, PAIRS_DEV, D), groups.reshape(N_DP, PAIRS_DEV)))
    pair_totals = lax.optimization_barrier(jnp.sum(term_blocks, axis=0))
    image_unit_grad = image_parts.reshape(PAIRS, D)
    text_unit_grad = scale_value * text_acc
    image_grad = (image_unit_grad - unit_image * lax.optimization_barrier(jnp.sum(unit_image * image_unit_grad, axis=1, keepdims=True))) / image_norm
    embed_grad = (text_unit_grad - unit_text * lax.optimization_barrier(jnp.sum(unit_text * text_unit_grad, axis=1, keepdims=True))) / text_norm
    gain_grad = lax.optimization_barrier(jnp.sum(embed_grad * pooled, axis=0))
    pooled_grad = embed_grad * text_gain[None, :]
    token_grad = jnp.take(pooled_grad, caption_ids, axis=0)
    scalars = pair_totals / float(PAIRS * PAIRS)
    return (image_grad, token_grad, gain_grad, scalars)
```

```python
import jax
import jax.numpy as jnp
from jax import lax
from jax.sharding import Mesh
from jax.sharding import PartitionSpec as P

Y, X, Z, C = ("dp_0", "dp_1", "dp_2", "dp_3")
DP = (Y, X, Z, C)
PLANE = (Y, X)
LANES = 128


def from_behind(value, by):
    count = lax.axis_size(DP)
    pairs = [(i, i + by) for i in range(count) if 0 <= i + by < count]
    return lax.ppermute(value, DP, pairs)


def exchange(value, axis, bit):
    return lax.ppermute(value, axis, [(i, i ^ bit) for i in range(lax.axis_size(axis))])


STEPS = ((Z, 4), (Z, 2), (Z, 1), (C, 1))


def unit_rows(values):
    length = jnp.sqrt(jnp.sum(values * values, axis=1, keepdims=True))
    return (values / length, length)


def to_plane(blocks):
    return lax.all_to_all(blocks, PLANE, 0, 0, tiled=True)


def per_device(image_emb, text_tokens, caption_ids, groups, text_gain, log_scale, logit_bias):
    f32, bf16 = jnp.float32, jnp.bfloat16
    pairs_here, width = image_emb.shape
    total_pairs = pairs_here * lax.axis_size(DP)
    plane = lax.axis_size(PLANE)
    first_pair = lax.axis_index(DP) * pairs_here
    scale_value = jnp.exp(log_scale[0])
    bias_value = logit_bias[0]

    lane = lax.broadcasted_iota(jnp.int32, (pairs_here, LANES), 1)
    id_lanes = jnp.where(
        lane == 0, (groups >> 8)[:, None], jnp.where(lane == 1, (groups & 255)[:, None], 0)
    ).astype(bf16)

    unit_image, image_norm = unit_rows(image_emb.astype(f32))
    images = jnp.concatenate([unit_image.astype(bf16), id_lanes], axis=1)
    for axis, bit in STEPS:
        images = jnp.concatenate([images, exchange(images, axis, bit)], axis=0)

    local_ids = caption_ids - first_pair
    slot = lax.broadcasted_iota(jnp.int32, (2 * pairs_here, 1), 0)
    wanted = jnp.where(slot < pairs_here, slot, jnp.where(slot == pairs_here, -1, -2))
    member = (local_ids[None, :] == wanted).astype(bf16)
    sums = jnp.dot(member, text_tokens, preferred_element_type=f32)
    arrived = from_behind(sums[pairs_here : pairs_here + 1], -1)
    last = lax.broadcasted_iota(jnp.int32, (pairs_here, 1), 0) == pairs_here - 1
    pooled = sums[:pairs_here] + jnp.where(last, arrived, 0.0)
    unit_text, text_norm = unit_rows(pooled * text_gain[None, :])
    text_rows = jnp.concatenate([unit_text.astype(bf16), id_lanes], axis=1)
    texts = to_plane(jnp.broadcast_to(text_rows[None], (plane,) + text_rows.shape))
    texts = texts.reshape(plane * pairs_here, width + LANES)

    image_low, text_low = images[:, :width], texts[:, :width]
    image_ids = images[:, width].astype(f32) * 256.0 + images[:, width + 1].astype(f32)
    text_ids = texts[:, width].astype(f32) * 256.0 + texts[:, width + 1].astype(f32)

    scaled = scale_value * lax.dot_general(
        image_low, text_low, (((1,), (1,)), ((), ())), preferred_element_type=f32
    )
    labels = jnp.where(image_ids[:, None] == text_ids[None, :], 1.0, -1.0).astype(f32)
    margin = -labels * (scaled + bias_value)
    coeffs = -labels * jax.nn.sigmoid(margin)
    sum_terms = jnp.stack(
        [jnp.sum(jax.nn.softplus(margin)), jnp.sum(coeffs * scaled), jnp.sum(coeffs)]
    )
    coeff_low = coeffs.astype(bf16)
    image_part = scale_value * jnp.dot(coeff_low, text_low, preferred_element_type=f32)
    text_part = scale_value * lax.dot_general(
        coeff_low, image_low, (((0,), (0,)), ((), ())), preferred_element_type=f32
    )

    text_back = to_plane(text_part.astype(bf16).reshape(plane, pairs_here, width))
    text_unit_grad = jnp.sum(text_back.astype(f32), axis=0)

    unit = text_low.astype(f32)
    along = jnp.sum(unit * text_part, axis=1, keepdims=True)
    gain_terms = jnp.sum((text_part - unit * along) * unit, axis=0) / text_gain
    totals = jnp.concatenate([gain_terms, sum_terms, jnp.zeros((LANES - 3,), f32)])[None]
    for axis, bit in reversed(STEPS):
        half = image_part.shape[0] // 2
        image_part = image_part[:half] + exchange(
            image_part[half:].astype(bf16), axis, bit
        ).astype(f32)
        totals = totals + exchange(totals, axis, bit)
    totals = jnp.sum(to_plane(jnp.broadcast_to(totals[None], (plane,) + totals.shape)), axis=0)[0]

    image_grad = (
        image_part - unit_image * jnp.sum(unit_image * image_part, axis=1, keepdims=True)
    ) / image_norm
    embed_grad = (
        text_unit_grad - unit_text * jnp.sum(unit_text * text_unit_grad, axis=1, keepdims=True)
    ) / text_norm
    pooled_grad = embed_grad * text_gain[None, :]
    behind = from_behind(pooled_grad[pairs_here - 1 :], 1)
    table = jnp.concatenate(
        [pooled_grad, behind, jnp.zeros((pairs_here - 1, width), f32)], axis=0
    )
    high = lax.reduce_precision(table, 8, 7)
    low = table - high
    parts = jnp.concatenate([high.astype(bf16), low.astype(bf16)], axis=0)
    token_grad = lax.dot_general(
        jnp.concatenate([member, member], axis=0),
        parts,
        (((0,), (0,)), ((), ())),
        preferred_element_type=f32,
    )
    gain_grad = totals[:width]
    scalars = totals[width : width + 3] / float(total_pairs * total_pairs)
    return (image_grad, token_grad, gain_grad, scalars)


def solution(mesh):
    finer = Mesh(mesh.devices.reshape(4, 4, 8, 2), DP)
    placed = (P(DP, None), P(DP, None), P(DP), P(DP), P(), P(), P())
    return jax.shard_map(
        per_device,
        mesh=finer,
        in_specs=placed,
        out_specs=(P(DP, None), P(DP, None), P(), P()),
        check_vma=False,
    )
```

```python
import jax
import jax.numpy as jnp
from jax import lax
from jax.experimental import pallas as pl
from jax.experimental.pallas import tpu as pltpu
from jax.sharding import Mesh
from jax.sharding import PartitionSpec as P

Y, X, Z, C = ("dp_0", "dp_1", "dp_2", "dp_3")
DP = (Y, X, Z, C)
PLANE = (Y, X)
LANES = 128
F32, BF16 = jnp.float32, jnp.bfloat16
SMEM = pl.BlockSpec(memory_space=pltpu.SMEM)
VMEM = pl.BlockSpec(memory_space=pltpu.VMEM)

STEPS = ((Z, 4), (Z, 2), (Z, 1), (C, 1))


def from_behind(value, by):
    count = lax.axis_size(DP)
    pairs = [(i, i + by) for i in range(count) if 0 <= i + by < count]
    return lax.ppermute(value, DP, pairs)


def exchange(value, axis, bit):
    return lax.ppermute(value, axis, [(i, i ^ bit) for i in range(lax.axis_size(axis))])


def to_plane(blocks):
    return lax.all_to_all(blocks, PLANE, 0, 0, tiled=True)


def members(ids, pairs, copies):
    slot = lax.broadcasted_iota(jnp.int32, (2 * pairs * copies, 1), 0) % (2 * pairs)
    last = ids[:, ids.shape[1] - 1 :]
    wanted = jnp.where(slot < pairs, slot - (pairs - 1), jnp.where(slot == pairs, -pairs, 1))
    return (ids - last == wanted).astype(F32).astype(BF16)


def id_tile(groups_ref, pairs, for_text):
    row = lax.broadcasted_iota(jnp.int32, (pairs, LANES), 0)
    lane = lax.broadcasted_iota(jnp.int32, (pairs, LANES), 1)
    ids = jnp.zeros((pairs, LANES), jnp.int32)
    for r in range(pairs):
        ids = jnp.where(row == r, groups_ref[r], ids)
    high, low = (ids >> 8) << 8, ids & 255
    if for_text:
        cells = jnp.where(lane < 2, 1, jnp.where(lane == 2, -high, jnp.where(lane == 3, -low, 0)))
    else:
        cells = jnp.where(lane == 0, high, jnp.where(lane == 1, low, jnp.where(lane < 4, 1, 0)))
    return cells.astype(F32).astype(BF16)


def prepare(groups_ref, ids_ref, image_ref, tokens_ref, row_ref, unit_ref, norm_ref, pooled_ref, spill_ref):
    pairs, width = image_ref.shape
    image = image_ref[...].astype(F32)
    norm = jnp.sqrt(jnp.sum(image * image, axis=1, keepdims=True))
    unit = image / norm
    unit_ref[...] = unit
    norm_ref[...] = norm
    row_ref[:, :width] = unit.astype(BF16)
    row_ref[:, width:] = id_tile(groups_ref, pairs, False)
    sums = jnp.dot(members(ids_ref[...], pairs, 1), tokens_ref[...], preferred_element_type=F32)
    pooled_ref[...] = sums[:pairs]
    spill_ref[...] = sums[pairs : pairs + 1]


def text_rows(groups_ref, pooled_ref, arrived_ref, gain_ref, rows_ref, unit_ref, norm_ref):
    pairs, width = pooled_ref.shape
    last = lax.broadcasted_iota(jnp.int32, (pairs, 1), 0) == pairs - 1
    pooled = pooled_ref[...] + jnp.where(last, arrived_ref[...], 0.0)
    embedded = pooled * gain_ref[...]
    norm = jnp.sqrt(jnp.sum(embedded * embedded, axis=1, keepdims=True))
    unit = embedded / norm
    unit_ref[...] = unit
    norm_ref[...] = norm
    low, ids = unit.astype(BF16), id_tile(groups_ref, pairs, True)
    for k in range(rows_ref.shape[0]):
        rows_ref[k, :, :width] = low
        rows_ref[k, :, width:] = ids


def pair_math(scalars_ref, image_ref, text_ref, gain_ref, text_out, keep_out, send_out):
    width = gain_ref.shape[1]
    scale = jnp.exp(jnp.full((1, LANES), scalars_ref[0], F32))[:, :1]
    image, text = image_ref[:, :width], text_ref[:, :width]
    contract = (((1,), (1,)), ((), ()))
    scaled = scale * lax.dot_general(image, text, contract, preferred_element_type=F32)
    apart = lax.dot_general(
        image_ref[:, width:], text_ref[:, width:], contract, preferred_element_type=F32
    )
    match = apart == 0.0
    logits = scaled + scalars_ref[1]
    margin = jnp.where(match, -logits, logits)
    tail = jnp.exp(-jnp.abs(margin))
    losses = jnp.maximum(margin, 0.0) + jnp.log1p(tail)
    sigmoid = jnp.where(margin >= 0.0, 1.0, tail) / (1.0 + tail)
    coeffs = jnp.where(match, -sigmoid, sigmoid)
    image_part = scale * jnp.dot(coeffs.astype(BF16), text, preferred_element_type=F32)
    text_part = scale * jnp.dot(coeffs.T.astype(BF16), image, preferred_element_type=F32)
    half = keep_out.shape[0]
    keep_out[...] = image_part[:half]
    send_out[...] = image_part[half:].astype(BF16)
    text_out[:, :width] = text_part.astype(BF16)

    unit = text.astype(F32)
    along = jnp.sum(unit * text_part, axis=1, keepdims=True)
    gain_terms = jnp.sum((text_part - unit * along) * unit, axis=0, keepdims=True) / gain_ref[...]
    row = lax.broadcasted_iota(jnp.int32, (8, LANES), 0)
    lane = lax.broadcasted_iota(jnp.int32, (8, LANES), 1)
    first = jnp.zeros((8, LANES), F32)
    for r in range(8):
        first = jnp.where(row == r, gain_terms[:, LANES * r : LANES * (r + 1)], first)
    second = jnp.where(row == 0, gain_terms[:, 8 * LANES : 9 * LANES], 0.0)
    for i, terms in enumerate((losses, coeffs * scaled, coeffs)):
        total = jnp.sum(jnp.sum(terms, axis=0, keepdims=True), axis=1, keepdims=True)
        high = total.astype(BF16).astype(F32)
        second = jnp.where((row == 1) & (lane == i), high, second)
        second = jnp.where((row == 2) & (lane == i), total - high, second)
    packed = jnp.concatenate([first, second], axis=1).astype(BF16)
    for k in range(text_out.shape[0] // 8):
        text_out[8 * k : 8 * (k + 1), width:] = packed


def text_gradient(back_ref, unit_ref, norm_ref, gain_ref, grad_out, last_out, totals_out):
    pairs, width = unit_ref.shape
    total = jnp.sum(back_ref[...].astype(F32), axis=0)
    totals_out[...] = total[:, width:]
    grad, unit = total[:, :width], unit_ref[...]
    grad = grad - unit * jnp.sum(unit * grad, axis=1, keepdims=True)
    grad = grad / norm_ref[...] * gain_ref[...]
    grad_out[...] = grad
    last_out[...] = grad[pairs - 1 :]


def finish(ids_ref, grad_ref, behind_ref, keep_ref, came_ref, unit_ref, norm_ref, token_out, image_out):
    pairs, width = grad_ref.shape
    table = jnp.concatenate(
        [grad_ref[...], jnp.broadcast_to(behind_ref[...], (pairs, width))], axis=0
    )
    high = table.astype(BF16)
    low = (table - high.astype(F32)).astype(BF16)
    token_out[...] = lax.dot_general(
        members(ids_ref[...], pairs, 2),
        jnp.concatenate([high, low], axis=0),
        (((0,), (0,)), ((), ())),
        preferred_element_type=F32,
    )
    grad, unit = keep_ref[...] + came_ref[...].astype(F32), unit_ref[...]
    grad = grad - unit * jnp.sum(unit * grad, axis=1, keepdims=True)
    image_out[...] = grad / norm_ref[...]


def local(kernel, specs, *outs):
    return pl.pallas_call(
        kernel,
        in_specs=specs,
        out_specs=[VMEM] * len(outs),
        out_shape=[jax.ShapeDtypeStruct(*o) for o in outs],
        compiler_params=pltpu.CompilerParams(vmem_limit_bytes=16 << 20),
    )


def per_device(image_emb, text_tokens, caption_ids, groups, text_gain, log_scale, logit_bias):
    pairs, width = image_emb.shape
    total_pairs = pairs * lax.axis_size(DP)
    plane = lax.axis_size(PLANE)
    wide = width + LANES
    ids = caption_ids[None, :]
    gain = text_gain[None, :]
    row, unit_image, image_norm, pooled, spill = local(
        prepare, [SMEM, VMEM, VMEM, VMEM],
        ((pairs, wide), BF16), ((pairs, width), F32), ((pairs, 1), F32), ((pairs, width), F32), ((1, width), F32),
    )(groups, ids, image_emb, text_tokens)

    arrived = from_behind(spill, -1)
    images = row
    for axis, bit in STEPS:
        images = jnp.concatenate([images, exchange(images, axis, bit)], axis=0)

    rows, unit_text, text_norm = local(
        text_rows, [SMEM, VMEM, VMEM, VMEM],
        ((plane, pairs, wide), BF16), ((pairs, width), F32), ((pairs, 1), F32),
    )(groups, pooled, arrived, gain)
    texts = to_plane(rows).reshape(plane * pairs, wide)

    line = images.shape[0]
    text_part, keep, send = local(
        pair_math, [SMEM, VMEM, VMEM, VMEM],
        ((plane * pairs, wide + LANES), BF16), ((line // 2, width), F32), ((line // 2, width), BF16),
    )(jnp.concatenate([log_scale, logit_bias]), images, texts, gain)

    back = to_plane(text_part.reshape(plane, pairs, wide + LANES))
    for n, (axis, bit) in enumerate(reversed(STEPS)):
        came = exchange(send, axis, bit)
        if n + 1 < len(STEPS):
            whole = keep + came.astype(F32)
            half = whole.shape[0] // 2
            keep, send = whole[:half], whole[half:].astype(BF16)

    pooled_grad, last, totals = local(
        text_gradient, [VMEM, VMEM, VMEM, VMEM],
        ((pairs, width), F32), ((1, width), F32), ((pairs, 2 * LANES), F32),
    )(back, unit_text, text_norm, gain)
    behind = from_behind(last, 1)
    for axis, bit in reversed(STEPS):
        totals = totals + exchange(totals, axis, bit)

    token_grad, image_grad = local(
        finish, [VMEM] * 7, ((text_tokens.shape[0], width), F32), ((pairs, width), F32)
    )(ids, pooled_grad, behind, keep, came, unit_image, image_norm)
    gain_grad = jnp.concatenate([totals[:, :LANES].reshape(-1), totals[0, LANES:]])
    scalars = (totals[1, LANES : LANES + 3] + totals[2, LANES : LANES + 3]) / float(
        total_pairs * total_pairs
    )
    return (image_grad, token_grad, gain_grad, scalars)


def solution(mesh):
    finer = Mesh(mesh.devices.reshape(4, 4, 8, 2), DP)
    placed = (P(DP, None), P(DP, None), P(DP), P(DP), P(), P(), P())
    return jax.shard_map(
        per_device,
        mesh=finer,
        in_specs=placed,
        out_specs=(P(DP, None), P(DP, None), P(), P()),
        check_vma=False,
    )
```

```python
import functools

import jax
import jax.numpy as jnp
from jax import lax
from jax.experimental import pallas as pl
from jax.experimental.pallas import tpu as pltpu
from jax.sharding import Mesh
from jax.sharding import PartitionSpec as P

Y, X, Z, C = ("dp_0", "dp_1", "dp_2", "dp_3")
DP = (Y, X, Z, C)
PLANE = (Y, X)
LANES = 128
F32, BF16 = jnp.float32, jnp.bfloat16
SMEM = pl.BlockSpec(memory_space=pltpu.SMEM)
VMEM = pl.BlockSpec(memory_space=pltpu.VMEM)
HBM = pl.BlockSpec(memory_space=pltpu.HBM)

STEPS = ((Z, 4), (Z, 2), (Z, 1), (C, 1))
FROM = (0, 4, 2, 6, 1, 5, 3, 7)


def from_behind(value, by):
    count = lax.axis_size(DP)
    pairs = [(i, i + by) for i in range(count) if 0 <= i + by < count]
    return lax.ppermute(value, DP, pairs)


def exchange(value, axis, bit):
    return lax.ppermute(value, axis, [(i, i ^ bit) for i in range(lax.axis_size(axis))])


def to_all(blocks, axes):
    return lax.all_to_all(blocks, axes, 0, 0, tiled=True)


def members(ids, pairs, copies):
    slot = lax.broadcasted_iota(jnp.int32, (2 * pairs * copies, 1), 0) % (2 * pairs)
    last = ids[:, ids.shape[1] - 1 :]
    wanted = jnp.where(slot < pairs, slot - (pairs - 1), jnp.where(slot == pairs, -pairs, 1))
    return (ids - last == wanted).astype(F32).astype(BF16)


def id_tile(groups_ref, pairs, for_text):
    row = lax.broadcasted_iota(jnp.int32, (pairs, LANES), 0)
    lane = lax.broadcasted_iota(jnp.int32, (pairs, LANES), 1)
    ids = jnp.zeros((pairs, LANES), jnp.int32)
    for r in range(pairs):
        ids = jnp.where(row == r, groups_ref[r], ids)
    high, low = (ids >> 8) << 8, ids & 255
    if for_text:
        cells = jnp.where(lane < 2, 1, jnp.where(lane == 2, -high, jnp.where(lane == 3, -low, 0)))
    else:
        cells = jnp.where(lane == 0, high, jnp.where(lane == 1, low, jnp.where(lane < 4, 1, 0)))
    return cells.astype(F32).astype(BF16)


def prepare(
    groups_hbm, ids_hbm, image_hbm, tokens_hbm, gain_hbm,
    row_ref, unit_ref, norm_ref, pooled_ref, spill_ref, tile_ref, gain_out,
    groups_ref, ids_ref, image_ref, tokens_ref, gain_ref, sems,
):
    pairs, width = image_hbm.shape
    moves = [
        pltpu.make_async_copy(source, target, sems.at[i])
        for i, (source, target) in enumerate(
            (
                (image_hbm, image_ref), (groups_hbm, groups_ref), (ids_hbm, ids_ref),
                (tokens_hbm, tokens_ref), (gain_hbm, gain_ref),
            )
        )
    ]
    for move in moves:
        move.start()
    moves[0].wait()
    moves[1].wait()
    image = image_ref[...].astype(F32)
    norm = jnp.sqrt(jnp.sum(image * image, axis=1, keepdims=True))
    unit = image / norm
    unit_ref[...] = unit
    norm_ref[...] = norm
    row_ref[:, :width] = unit.astype(BF16)
    row_ref[:, width:] = id_tile(groups_ref, pairs, False)
    tile_ref[...] = id_tile(groups_ref, pairs, True)
    moves[4].wait()
    gain_out[...] = gain_ref[...][None, :]
    moves[2].wait()
    moves[3].wait()
    sums = jnp.dot(members(ids_ref[...], pairs, 1), tokens_ref[...], preferred_element_type=F32)
    pooled_ref[...] = sums[:pairs]
    spill_ref[...] = sums[pairs : pairs + 1]


def text_rows(tile_ref, pooled_ref, arrived_ref, gain_ref, rows_ref, unit_ref, norm_ref):
    pairs, width = pooled_ref.shape
    last = lax.broadcasted_iota(jnp.int32, (pairs, 1), 0) == pairs - 1
    pooled = pooled_ref[...] + jnp.where(last, arrived_ref[...], 0.0)
    embedded = pooled * gain_ref[...]
    norm = jnp.sqrt(jnp.sum(embedded * embedded, axis=1, keepdims=True))
    unit = embedded / norm
    unit_ref[...] = unit
    norm_ref[...] = norm
    low, ids = unit.astype(BF16), tile_ref[...]
    for k in range(rows_ref.shape[0]):
        rows_ref[k, :, :width] = low
        rows_ref[k, :, width:] = ids


def pair_math(log_scale_ref, bias_ref, image_ref, text_ref, gain_ref, text_out, keep_out, send_out):
    width = gain_ref.shape[1]
    scale = jnp.exp(jnp.full((1, LANES), log_scale_ref[0], F32))[:, :1]
    image, text = image_ref[:, :width], text_ref[:, :width]
    contract = (((1,), (1,)), ((), ()))
    scaled = scale * lax.dot_general(image, text, contract, preferred_element_type=F32)
    apart = lax.dot_general(
        image_ref[:, width:], text_ref[:, width:], contract, preferred_element_type=F32
    )
    match = apart == 0.0
    logits = scaled + bias_ref[0]
    margin = jnp.where(match, -logits, logits)
    tail = jnp.exp(-jnp.abs(margin))
    losses = jnp.maximum(margin, 0.0) + jnp.log1p(tail)
    sigmoid = jnp.where(margin >= 0.0, 1.0, tail) / (1.0 + tail)
    coeffs = jnp.where(match, -sigmoid, sigmoid)
    image_part = scale * jnp.dot(coeffs.astype(BF16), text, preferred_element_type=F32)
    text_part = scale * jnp.dot(coeffs.T.astype(BF16), image, preferred_element_type=F32)
    half = keep_out.shape[0]
    keep_out[...] = image_part[:half]
    send_out[...] = image_part[half:].astype(BF16)
    text_out[:, :width] = text_part.astype(BF16)

    unit = text.astype(F32)
    along = jnp.sum(unit * text_part, axis=1, keepdims=True)
    gain_terms = jnp.sum((text_part - unit * along) * unit, axis=0, keepdims=True) / gain_ref[...]
    row = lax.broadcasted_iota(jnp.int32, (8, LANES), 0)
    lane = lax.broadcasted_iota(jnp.int32, (8, LANES), 1)
    first = jnp.zeros((8, LANES), F32)
    for r in range(8):
        first = jnp.where(row == r, gain_terms[:, LANES * r : LANES * (r + 1)], first)
    second = jnp.where(row == 0, gain_terms[:, 8 * LANES : 9 * LANES], 0.0)
    for i, terms in enumerate((losses, coeffs * scaled, coeffs)):
        total = jnp.sum(jnp.sum(terms, axis=0, keepdims=True), axis=1, keepdims=True)
        high = total.astype(BF16).astype(F32)
        second = jnp.where((row == 1) & (lane == i), high, second)
        second = jnp.where((row == 2) & (lane == i), total - high, second)
    packed = jnp.concatenate([first, second], axis=1).astype(BF16)
    for k in range(text_out.shape[0] // 8):
        text_out[8 * k : 8 * (k + 1), width:] = packed


def text_gradient(back_ref, unit_ref, norm_ref, gain_ref, grad_out, last_out, totals_out):
    pairs, width = unit_ref.shape
    total = jnp.sum(back_ref[...].astype(F32), axis=0)
    totals_out[...] = total[:, width:]
    grad, unit = total[:, :width], unit_ref[...]
    grad = grad - unit * jnp.sum(unit * grad, axis=1, keepdims=True)
    grad = grad / norm_ref[...] * gain_ref[...]
    grad_out[...] = grad
    last_out[...] = grad[pairs - 1 :]


def pack(place_ref, keep_ref, came_ref, totals_ref, other_ref, out_ref):
    places, pairs, _ = out_ref.shape
    width = keep_ref.shape[1]
    total = totals_ref[...] + other_ref[...]
    high = total.astype(BF16)
    low = (total - high.astype(F32)).astype(BF16)
    for k in range(places):
        rows = slice(pairs * k, pairs * (k + 1))
        block = keep_ref[rows] + came_ref[rows].astype(F32)
        place = place_ref[0] ^ FROM[k]
        out_ref[place, :, :width] = block.astype(BF16)
        out_ref[place, :, width : width + 2 * LANES] = high
        out_ref[place, :, width + 2 * LANES :] = low


def token_rows(ids_ref, grad_ref, behind_ref, token_out):
    pairs, width = grad_ref.shape
    table = jnp.concatenate(
        [grad_ref[...], jnp.broadcast_to(behind_ref[...], (pairs, width))], axis=0
    )
    high = table.astype(BF16)
    low = (table - high.astype(F32)).astype(BF16)
    token_out[...] = lax.dot_general(
        members(ids_ref[...], pairs, 2),
        jnp.concatenate([high, low], axis=0),
        (((0,), (0,)), ((), ())),
        preferred_element_type=F32,
    )


def finish(back_ref, unit_ref, norm_ref, image_out, gain_out, scalars_out, *, count):
    width = unit_ref.shape[1]
    total = jnp.sum(back_ref[...].astype(F32), axis=0)
    first = total[:, width : width + LANES] + total[:, width + 2 * LANES : width + 3 * LANES]
    second = total[:, width + LANES : width + 2 * LANES] + total[:, width + 3 * LANES :]
    gain_out[...] = jnp.concatenate([first[r] for r in range(8)] + [second[0]])
    scalars_out[...] = ((second[1] + second[2]) / count)[:3]
    grad, unit = total[:, :width], unit_ref[...]
    grad = grad - unit * jnp.sum(unit * grad, axis=1, keepdims=True)
    image_out[...] = grad / norm_ref[...]


def local(kernel, specs, *outs, scratch=()):
    return pl.pallas_call(
        kernel,
        in_specs=specs,
        out_specs=[VMEM] * len(outs),
        out_shape=[jax.ShapeDtypeStruct(*o) for o in outs],
        scratch_shapes=scratch,
        compiler_params=pltpu.CompilerParams(vmem_limit_bytes=16 << 20),
    )


def per_device(image_emb, text_tokens, caption_ids, groups, text_gain, log_scale, logit_bias):
    pairs, width = image_emb.shape
    tokens = text_tokens.shape[0]
    total_pairs = pairs * lax.axis_size(DP)
    plane = lax.axis_size(PLANE)
    wide = width + LANES
    ids = caption_ids[None, :]
    row, unit_image, image_norm, pooled, spill, tile, gain = local(
        prepare, [HBM] * 5,
        ((pairs, wide), BF16), ((pairs, width), F32), ((pairs, 1), F32), ((pairs, width), F32), ((1, width), F32),
        ((pairs, LANES), BF16), ((1, width), F32),
        scratch=(
            pltpu.SMEM((pairs,), jnp.int32), pltpu.VMEM((1, tokens), jnp.int32),
            pltpu.VMEM((pairs, width), BF16), pltpu.VMEM((tokens, width), BF16),
            pltpu.VMEM((width,), F32), pltpu.SemaphoreType.DMA((5,)),
        ),
    )(*(pltpu.with_memory_space_constraint(a, pltpu.HBM) for a in (groups, ids, image_emb, text_tokens, text_gain)))

    arrived = from_behind(spill, -1)
    images = row
    for axis, bit in STEPS:
        images = jnp.concatenate([images, exchange(images, axis, bit)], axis=0)

    rows, unit_text, text_norm = local(
        text_rows, [VMEM] * 4,
        ((plane, pairs, wide), BF16), ((pairs, width), F32), ((pairs, 1), F32),
    )(tile, pooled, arrived, gain)
    texts = to_all(rows, PLANE).reshape(plane * pairs, wide)

    line = images.shape[0]
    text_part, keep, send = local(
        pair_math, [SMEM, SMEM, VMEM, VMEM, VMEM],
        ((plane * pairs, wide + LANES), BF16), ((line // 2, width), F32), ((line // 2, width), BF16),
    )(log_scale, logit_bias, images, texts, gain)

    back = to_all(text_part.reshape(plane, pairs, wide + LANES), PLANE)
    came = exchange(send, C, 1)
    pooled_grad, last, totals = local(
        text_gradient, [VMEM, VMEM, VMEM, VMEM],
        ((pairs, width), F32), ((1, width), F32), ((pairs, 2 * LANES), F32),
    )(back, unit_text, text_norm, gain)
    other = exchange(totals, C, 1)
    depth = lax.axis_size(Z)
    (blocks,) = local(
        pack, [SMEM, VMEM, VMEM, VMEM, VMEM], ((depth, pairs, width + 4 * LANES), BF16)
    )(lax.axis_index(Z)[None], keep, came, totals, other)
    line_back = to_all(blocks, Z)
    behind = from_behind(last, 1)
    (token_grad,) = local(token_rows, [VMEM] * 3, ((tokens, width), F32))(ids, pooled_grad, behind)
    image_grad, gain_grad, scalars = local(
        functools.partial(finish, count=float(total_pairs * total_pairs)), [VMEM] * 3,
        ((pairs, width), F32), ((width,), F32), ((3,), F32),
    )(line_back, unit_image, image_norm)
    return (image_grad, token_grad, gain_grad, scalars)


def solution(mesh):
    finer = Mesh(mesh.devices.reshape(4, 4, 8, 2), DP)
    placed = (P(DP, None), P(DP, None), P(DP), P(DP), P(), P(), P())
    return jax.shard_map(
        per_device,
        mesh=finer,
        in_specs=placed,
        out_specs=(P(DP, None), P(DP, None), P(), P()),
        check_vma=False,
    )
```

```python
import functools

import jax
import jax.numpy as jnp
from jax import lax
from jax.experimental import pallas as pl
from jax.experimental.pallas import tpu as pltpu
from jax.sharding import Mesh
from jax.sharding import PartitionSpec as P

Y, X, Z, C = ("dp_0", "dp_1", "dp_2", "dp_3")
DP = (Y, X, Z, C)
PLANE = (Y, X)
LANES = 128
F32, BF16 = jnp.float32, jnp.bfloat16
VMEM = pl.BlockSpec(memory_space=pltpu.VMEM)
HBM = pl.BlockSpec(memory_space=pltpu.HBM)


def from_behind(value, by):
    count = lax.axis_size(DP)
    pairs = [(i, i + by) for i in range(count) if 0 <= i + by < count]
    return lax.ppermute(value, DP, pairs)


def exchange(value, axis, bit):
    return lax.ppermute(value, axis, [(i, i ^ bit) for i in range(lax.axis_size(axis))])


def to_all(blocks, axes):
    return lax.all_to_all(blocks, axes, 0, 0, tiled=True)


def members(ids, pairs, copies):
    slot = lax.broadcasted_iota(jnp.int32, (2 * pairs * copies, 1), 0) % (2 * pairs)
    last = ids[:, ids.shape[1] - 1 :]
    wanted = jnp.where(slot < pairs, slot - (pairs - 1), jnp.where(slot == pairs, -pairs, 1))
    return (ids - last == wanted).astype(F32).astype(BF16)


def id_tile(groups_ref, pairs, for_text):
    row = lax.broadcasted_iota(jnp.int32, (pairs, LANES), 0)
    lane = lax.broadcasted_iota(jnp.int32, (pairs, LANES), 1)
    ids = jnp.zeros((pairs, LANES), jnp.int32)
    for r in range(pairs):
        ids = jnp.where(row == r, groups_ref[r], ids)
    high, low = (ids >> 8) << 8, ids & 255
    if for_text:
        cells = jnp.where(lane < 2, 1, jnp.where(lane == 2, -high, jnp.where(lane == 3, -low, 0)))
    else:
        cells = jnp.where(lane == 0, high, jnp.where(lane == 1, low, jnp.where(lane < 4, 1, 0)))
    return cells.astype(F32).astype(BF16)


def repeat(rows_ref, features, ids):
    width = features.shape[1]
    for k in range(rows_ref.shape[0]):
        rows_ref[k, :, :width] = features
        rows_ref[k, :, width:] = ids


def prepare(
    groups_hbm, ids_hbm, image_hbm, tokens_hbm, gain_hbm,
    rows_ref, unit_ref, norm_ref, pooled_ref, spill_ref, tile_ref, gain_out,
    groups_ref, ids_ref, image_ref, tokens_ref, gain_ref, sems,
):
    pairs, _ = image_hbm.shape
    moves = [
        pltpu.make_async_copy(source, target, sems.at[i])
        for i, (source, target) in enumerate(
            (
                (image_hbm, image_ref), (groups_hbm, groups_ref), (ids_hbm, ids_ref),
                (tokens_hbm, tokens_ref), (gain_hbm, gain_ref),
            )
        )
    ]
    for move in moves:
        move.start()
    moves[0].wait()
    moves[1].wait()
    image = image_ref[...].astype(F32)
    norm = jnp.sqrt(jnp.sum(image * image, axis=1, keepdims=True))
    unit = image / norm
    unit_ref[...] = unit
    norm_ref[...] = norm
    repeat(rows_ref, unit.astype(BF16), id_tile(groups_ref, pairs, False))
    tile_ref[...] = id_tile(groups_ref, pairs, True)
    moves[4].wait()
    gain_out[...] = gain_ref[...][None, :]
    moves[2].wait()
    moves[3].wait()
    sums = jnp.dot(members(ids_ref[...], pairs, 1), tokens_ref[...], preferred_element_type=F32)
    pooled_ref[...] = sums[:pairs]
    spill_ref[...] = sums[pairs : pairs + 1]


def text_rows(tile_ref, pooled_ref, arrived_ref, gain_ref, rows_ref, unit_ref, norm_ref):
    pairs, _ = pooled_ref.shape
    last = lax.broadcasted_iota(jnp.int32, (pairs, 1), 0) == pairs - 1
    pooled = pooled_ref[...] + jnp.where(last, arrived_ref[...], 0.0)
    embedded = pooled * gain_ref[...]
    norm = jnp.sqrt(jnp.sum(embedded * embedded, axis=1, keepdims=True))
    unit = embedded / norm
    unit_ref[...] = unit
    norm_ref[...] = norm
    repeat(rows_ref, unit.astype(BF16), tile_ref[...])


def pair_math(knobs_ref, near_ref, far_ref, text_ref, gain_ref, text_out, keep_out, send_out):
    width = gain_ref.shape[1]
    scale = jnp.exp(knobs_ref[:, :1])
    rows = jnp.concatenate([near_ref[...], far_ref[...]], axis=0)
    image, text = rows[:, :width], text_ref[:, :width]
    contract = (((1,), (1,)), ((), ()))
    scaled = scale * lax.dot_general(image, text, contract, preferred_element_type=F32)
    apart = lax.dot_general(
        rows[:, width:], text_ref[:, width:], contract, preferred_element_type=F32
    )
    match = apart == 0.0
    logits = scaled + knobs_ref[:, 1:2]
    margin = jnp.where(match, -logits, logits)
    tail = jnp.exp(-jnp.abs(margin))
    losses = jnp.maximum(margin, 0.0) + jnp.log1p(tail)
    sigmoid = jnp.where(margin >= 0.0, 1.0, tail) / (1.0 + tail)
    coeffs = jnp.where(match, -sigmoid, sigmoid)
    image_part = scale * jnp.dot(coeffs.astype(BF16), text, preferred_element_type=F32)
    text_part = scale * jnp.dot(coeffs.T.astype(BF16), image, preferred_element_type=F32)
    half = keep_out.shape[0]
    keep_out[...] = image_part[:half]
    send_out[...] = image_part[half:].astype(BF16)
    text_out[:, :width] = text_part.astype(BF16)

    unit = text.astype(F32)
    along = jnp.sum(unit * text_part, axis=1, keepdims=True)
    gain_terms = jnp.sum((text_part - unit * along) * unit, axis=0, keepdims=True) / gain_ref[...]
    row = lax.broadcasted_iota(jnp.int32, (8, LANES), 0)
    lane = lax.broadcasted_iota(jnp.int32, (8, LANES), 1)
    first = jnp.zeros((8, LANES), F32)
    for r in range(8):
        first = jnp.where(row == r, gain_terms[:, LANES * r : LANES * (r + 1)], first)
    second = jnp.where(row == 0, gain_terms[:, 8 * LANES : 9 * LANES], 0.0)
    for i, terms in enumerate((losses, coeffs * scaled, coeffs)):
        total = jnp.sum(jnp.sum(terms, axis=0, keepdims=True), axis=1, keepdims=True)
        high = total.astype(BF16).astype(F32)
        second = jnp.where((row == 1) & (lane == i), high, second)
        second = jnp.where((row == 2) & (lane == i), total - high, second)
    packed = jnp.concatenate([first, second], axis=1).astype(BF16)
    for k in range(text_out.shape[0] // 8):
        text_out[8 * k : 8 * (k + 1), width:] = packed


def text_gradient(back_ref, unit_ref, norm_ref, gain_ref, grad_out, last_out, totals_out):
    pairs, width = unit_ref.shape
    total = jnp.sum(back_ref[...].astype(F32), axis=0)
    totals_out[...] = total[:, width:]
    grad, unit = total[:, :width], unit_ref[...]
    grad = grad - unit * jnp.sum(unit * grad, axis=1, keepdims=True)
    grad = grad / norm_ref[...] * gain_ref[...]
    grad_out[...] = grad
    last_out[...] = grad[pairs - 1 :]


def pack(keep_ref, came_ref, totals_ref, other_ref, out_ref):
    places, pairs, _ = out_ref.shape
    width = keep_ref.shape[1]
    total = totals_ref[...] + other_ref[...]
    high = total.astype(BF16)
    low = (total - high.astype(F32)).astype(BF16)
    for k in range(places):
        rows = slice(pairs * k, pairs * (k + 1))
        block = keep_ref[rows] + came_ref[rows].astype(F32)
        out_ref[k, :, :width] = block.astype(BF16)
        out_ref[k, :, width : width + 2 * LANES] = high
        out_ref[k, :, width + 2 * LANES :] = low


def token_rows(ids_ref, grad_ref, behind_ref, token_out):
    pairs, width = grad_ref.shape
    table = jnp.concatenate(
        [grad_ref[...], jnp.broadcast_to(behind_ref[...], (pairs, width))], axis=0
    )
    high = table.astype(BF16)
    low = (table - high.astype(F32)).astype(BF16)
    token_out[...] = lax.dot_general(
        members(ids_ref[...], pairs, 2),
        jnp.concatenate([high, low], axis=0),
        (((0,), (0,)), ((), ())),
        preferred_element_type=F32,
    )


def finish(back_ref, unit_ref, norm_ref, image_out, gain_out, scalars_out, *, count):
    width = unit_ref.shape[1]
    total = jnp.sum(back_ref[...].astype(F32), axis=0)
    first = total[:, width : width + LANES] + total[:, width + 2 * LANES : width + 3 * LANES]
    second = total[:, width + LANES : width + 2 * LANES] + total[:, width + 3 * LANES :]
    gain_out[...] = jnp.concatenate([first[r] for r in range(8)] + [second[0]])
    scalars_out[...] = ((second[1] + second[2]) / count)[:3]
    grad, unit = total[:, :width], unit_ref[...]
    grad = grad - unit * jnp.sum(unit * grad, axis=1, keepdims=True)
    image_out[...] = grad / norm_ref[...]


def local(kernel, specs, *outs, scratch=()):
    return pl.pallas_call(
        kernel,
        in_specs=specs,
        out_specs=[VMEM] * len(outs),
        out_shape=[jax.ShapeDtypeStruct(*o) for o in outs],
        scratch_shapes=scratch,
        compiler_params=pltpu.CompilerParams(vmem_limit_bytes=16 << 20),
    )


def per_device(image_emb, text_tokens, caption_ids, groups, text_gain, log_scale, logit_bias):
    pairs, width = image_emb.shape
    tokens = text_tokens.shape[0]
    total_pairs = pairs * lax.axis_size(DP)
    plane, depth = lax.axis_size(PLANE), lax.axis_size(Z)
    wide = width + LANES
    ids = caption_ids[None, :]
    near, unit_image, image_norm, pooled, spill, tile, gain = local(
        prepare, [HBM] * 5,
        ((depth, pairs, wide), BF16), ((pairs, width), F32), ((pairs, 1), F32), ((pairs, width), F32),
        ((1, width), F32), ((pairs, LANES), BF16), ((1, width), F32),
        scratch=(
            pltpu.SMEM((pairs,), jnp.int32), pltpu.VMEM((1, tokens), jnp.int32),
            pltpu.VMEM((pairs, width), BF16), pltpu.VMEM((tokens, width), BF16), pltpu.VMEM((width,), F32),
            pltpu.SemaphoreType.DMA((5,)),
        ),
    )(
        *(
            pltpu.with_memory_space_constraint(a, pltpu.HBM)
            for a in (groups, ids, image_emb, text_tokens, text_gain)
        )
    )

    near = to_all(near, Z).reshape(depth * pairs, wide)
    arrived = from_behind(spill, -1)
    rows, unit_text, text_norm = local(
        text_rows, [VMEM] * 4,
        ((plane, pairs, wide), BF16), ((pairs, width), F32), ((pairs, 1), F32),
    )(tile, pooled, arrived, gain)
    texts = to_all(rows, PLANE).reshape(plane * pairs, wide)

    far = exchange(near, C, 1)
    far, log_scale, logit_bias = lax.optimization_barrier((far, log_scale, logit_bias))
    lane = lax.broadcasted_iota(jnp.int32, (1, LANES), 1)
    knobs = jnp.where(lane == 0, log_scale[0], logit_bias[0])
    text_part, keep, send = local(
        pair_math, [VMEM] * 5,
        ((plane * pairs, wide + LANES), BF16), ((depth * pairs, width), F32), ((depth * pairs, width), BF16),
    )(knobs, near, far, texts, gain)

    back = to_all(text_part.reshape(plane, pairs, wide + LANES), PLANE)
    came = exchange(send, C, 1)
    pooled_grad, last, totals = local(
        text_gradient, [VMEM, VMEM, VMEM, VMEM],
        ((pairs, width), F32), ((1, width), F32), ((pairs, 2 * LANES), F32),
    )(back, unit_text, text_norm, gain)
    other = exchange(totals, C, 1)
    (blocks,) = local(pack, [VMEM] * 4, ((depth, pairs, width + 4 * LANES), BF16))(
        keep, came, totals, other
    )
    line_back = to_all(blocks, Z)
    behind = from_behind(last, 1)
    (token_grad,) = local(token_rows, [VMEM] * 3, ((tokens, width), F32))(ids, pooled_grad, behind)
    image_grad, gain_grad, scalars = local(
        functools.partial(finish, count=float(total_pairs * total_pairs)), [VMEM] * 3,
        ((pairs, width), F32), ((width,), F32), ((3,), F32),
    )(line_back, unit_image, image_norm)
    return (image_grad, token_grad, gain_grad, scalars)


def solution(mesh):
    finer = Mesh(mesh.devices.reshape(4, 4, 8, 2), DP)
    placed = (P(DP, None), P(DP, None), P(DP), P(DP), P(), P(), P())
    return jax.shard_map(
        per_device,
        mesh=finer,
        in_specs=placed,
        out_specs=(P(DP, None), P(DP, None), P(), P()),
        check_vma=False,
    )
```

```python
import functools

import jax
import jax.numpy as jnp
from jax import lax
from jax.experimental import pallas as pl
from jax.experimental.pallas import tpu as pltpu
from jax.sharding import Mesh
from jax.sharding import PartitionSpec as P

Y, X, Z, C = ("dp_0", "dp_1", "dp_2", "dp_3")
DP = (Y, X, Z, C)
PLANE = (Y, X)
LANES = 128
F32, BF16 = jnp.float32, jnp.bfloat16
VMEM = pl.BlockSpec(memory_space=pltpu.VMEM)
SMEM = pl.BlockSpec(memory_space=pltpu.SMEM)
HBM = pl.BlockSpec(memory_space=pltpu.HBM)

FROM = (0, 2, 4, 6, 1, 3, 5, 7)


def from_behind(value, by):
    count = lax.axis_size(DP)
    pairs = [(i, i + by) for i in range(count) if 0 <= i + by < count]
    return lax.ppermute(value, DP, pairs)


def exchange(value, axis, bit):
    return lax.ppermute(value, axis, [(i, i ^ bit) for i in range(lax.axis_size(axis))])


def to_all(blocks, axes):
    return lax.all_to_all(blocks, axes, 0, 0, tiled=True)


def members(ids, pairs, copies):
    slot = lax.broadcasted_iota(jnp.int32, (2 * pairs * copies, 1), 0) % (2 * pairs)
    last = ids[:, ids.shape[1] - 1 :]
    wanted = jnp.where(slot < pairs, slot - (pairs - 1), jnp.where(slot == pairs, -pairs, 1))
    return (ids - last == wanted).astype(F32).astype(BF16)


def id_tile(groups_ref, pairs, for_text):
    row = lax.broadcasted_iota(jnp.int32, (pairs, LANES), 0)
    lane = lax.broadcasted_iota(jnp.int32, (pairs, LANES), 1)
    ids = jnp.zeros((pairs, LANES), jnp.int32)
    for r in range(pairs):
        ids = jnp.where(row == r, groups_ref[r], ids)
    high, low = (ids >> 8) << 8, ids & 255
    if for_text:
        cells = jnp.where(lane < 2, 1, jnp.where(lane == 2, -high, jnp.where(lane == 3, -low, 0)))
    else:
        cells = jnp.where(lane == 0, high, jnp.where(lane == 1, low, jnp.where(lane < 4, 1, 0)))
    return cells.astype(F32).astype(BF16)


def prepare(
    groups_hbm, ids_hbm, image_hbm, tokens_hbm, gain_hbm,
    row_ref, unit_ref, norm_ref, pooled_ref, spill_ref, tile_ref, gain_out,
    groups_ref, ids_ref, image_ref, tokens_ref, gain_ref, sems,
):
    pairs, width = image_hbm.shape
    moves = [
        pltpu.make_async_copy(source, target, sems.at[i])
        for i, (source, target) in enumerate(
            (
                (image_hbm, image_ref), (groups_hbm, groups_ref), (ids_hbm, ids_ref),
                (tokens_hbm, tokens_ref), (gain_hbm, gain_ref),
            )
        )
    ]
    for move in moves:
        move.start()
    moves[0].wait()
    moves[1].wait()
    image = image_ref[...].astype(F32)
    norm = jnp.sqrt(jnp.sum(image * image, axis=1, keepdims=True))
    unit = image / norm
    unit_ref[...] = unit
    norm_ref[...] = norm
    row_ref[:, :width] = unit.astype(BF16)
    row_ref[:, width:] = id_tile(groups_ref, pairs, False)
    tile_ref[...] = id_tile(groups_ref, pairs, True)
    moves[4].wait()
    gain_out[...] = gain_ref[...][None, :]
    moves[2].wait()
    moves[3].wait()
    sums = jnp.dot(members(ids_ref[...], pairs, 1), tokens_ref[...], preferred_element_type=F32)
    pooled_ref[...] = sums[:pairs]
    spill_ref[...] = sums[pairs : pairs + 1]


def text_rows(tile_ref, pooled_ref, arrived_ref, gain_ref, rows_ref, unit_ref, norm_ref):
    pairs, width = pooled_ref.shape
    last = lax.broadcasted_iota(jnp.int32, (pairs, 1), 0) == pairs - 1
    pooled = pooled_ref[...] + jnp.where(last, arrived_ref[...], 0.0)
    embedded = pooled * gain_ref[...]
    norm = jnp.sqrt(jnp.sum(embedded * embedded, axis=1, keepdims=True))
    unit = embedded / norm
    unit_ref[...] = unit
    norm_ref[...] = norm
    low, ids = unit.astype(BF16), tile_ref[...]
    for k in range(rows_ref.shape[0]):
        rows_ref[k, :, :width] = low
        rows_ref[k, :, width:] = ids


def pair_math(knobs_ref, near_ref, far_ref, text_ref, gain_ref, text_out, keep_out, send_out):
    width = gain_ref.shape[1]
    scale = jnp.exp(knobs_ref[:, :1])
    rows = jnp.concatenate([near_ref[...], far_ref[...]], axis=0)
    image, text = rows[:, :width], text_ref[:, :width]
    contract = (((1,), (1,)), ((), ()))
    scaled = scale * lax.dot_general(image, text, contract, preferred_element_type=F32)
    apart = lax.dot_general(
        rows[:, width:], text_ref[:, width:], contract, preferred_element_type=F32
    )
    match = apart == 0.0
    logits = scaled + knobs_ref[:, 1:2]
    margin = jnp.where(match, -logits, logits)
    tail = jnp.exp(-jnp.abs(margin))
    losses = jnp.maximum(margin, 0.0) + jnp.log1p(tail)
    sigmoid = jnp.where(margin >= 0.0, 1.0, tail) / (1.0 + tail)
    coeffs = jnp.where(match, -sigmoid, sigmoid)
    image_part = scale * jnp.dot(coeffs.astype(BF16), text, preferred_element_type=F32)
    text_part = scale * jnp.dot(coeffs.T.astype(BF16), image, preferred_element_type=F32)
    half = keep_out.shape[0]
    keep_out[...] = image_part[:half]
    send_out[...] = image_part[half:].astype(BF16)
    text_out[:, :width] = text_part.astype(BF16)

    unit = text.astype(F32)
    along = jnp.sum(unit * text_part, axis=1, keepdims=True)
    gain_terms = jnp.sum((text_part - unit * along) * unit, axis=0, keepdims=True) / gain_ref[...]
    row = lax.broadcasted_iota(jnp.int32, (8, LANES), 0)
    lane = lax.broadcasted_iota(jnp.int32, (8, LANES), 1)
    first = jnp.zeros((8, LANES), F32)
    for r in range(8):
        first = jnp.where(row == r, gain_terms[:, LANES * r : LANES * (r + 1)], first)
    second = jnp.where(row == 0, gain_terms[:, 8 * LANES : 9 * LANES], 0.0)
    for i, terms in enumerate((losses, coeffs * scaled, coeffs)):
        total = jnp.sum(jnp.sum(terms, axis=0, keepdims=True), axis=1, keepdims=True)
        high = total.astype(BF16).astype(F32)
        second = jnp.where((row == 1) & (lane == i), high, second)
        second = jnp.where((row == 2) & (lane == i), total - high, second)
    packed = jnp.concatenate([first, second], axis=1).astype(BF16)
    for k in range(text_out.shape[0] // 8):
        text_out[8 * k : 8 * (k + 1), width:] = packed


def text_gradient(back_ref, unit_ref, norm_ref, gain_ref, grad_out, last_out, totals_out):
    pairs, width = unit_ref.shape
    total = jnp.sum(back_ref[...].astype(F32), axis=0)
    totals_out[...] = total[:, width:]
    grad, unit = total[:, :width], unit_ref[...]
    grad = grad - unit * jnp.sum(unit * grad, axis=1, keepdims=True)
    grad = grad / norm_ref[...] * gain_ref[...]
    grad_out[...] = grad
    last_out[...] = grad[pairs - 1 :]


def pack(place_ref, keep_ref, came_ref, totals_ref, other_ref, out_ref):
    places, pairs, _ = out_ref.shape
    width = keep_ref.shape[1]
    total = totals_ref[...] + other_ref[...]
    high = total.astype(BF16)
    low = (total - high.astype(F32)).astype(BF16)
    for k in range(places):
        rows = slice(pairs * k, pairs * (k + 1))
        block = keep_ref[rows] + came_ref[rows].astype(F32)
        place = place_ref[0] ^ FROM[k]
        out_ref[place, :, :width] = block.astype(BF16)
        out_ref[place, :, width : width + 2 * LANES] = high
        out_ref[place, :, width + 2 * LANES :] = low


def token_rows(ids_ref, grad_ref, behind_ref, token_out):
    pairs, width = grad_ref.shape
    table = jnp.concatenate(
        [grad_ref[...], jnp.broadcast_to(behind_ref[...], (pairs, width))], axis=0
    )
    high = table.astype(BF16)
    low = (table - high.astype(F32)).astype(BF16)
    token_out[...] = lax.dot_general(
        members(ids_ref[...], pairs, 2),
        jnp.concatenate([high, low], axis=0),
        (((0,), (0,)), ((), ())),
        preferred_element_type=F32,
    )


def finish(back_ref, unit_ref, norm_ref, image_out, gain_out, scalars_out, *, count):
    width = unit_ref.shape[1]
    total = jnp.sum(back_ref[...].astype(F32), axis=0)
    first = total[:, width : width + LANES] + total[:, width + 2 * LANES : width + 3 * LANES]
    second = total[:, width + LANES : width + 2 * LANES] + total[:, width + 3 * LANES :]
    gain_out[...] = jnp.concatenate([first[r] for r in range(8)] + [second[0]])
    scalars_out[...] = ((second[1] + second[2]) / count)[:3]
    grad, unit = total[:, :width], unit_ref[...]
    grad = grad - unit * jnp.sum(unit * grad, axis=1, keepdims=True)
    image_out[...] = grad / norm_ref[...]


def local(kernel, specs, *outs, scratch=()):
    return pl.pallas_call(
        kernel,
        in_specs=specs,
        out_specs=[VMEM] * len(outs),
        out_shape=[jax.ShapeDtypeStruct(*o) for o in outs],
        scratch_shapes=scratch,
        compiler_params=pltpu.CompilerParams(vmem_limit_bytes=16 << 20),
    )


def per_device(image_emb, text_tokens, caption_ids, groups, text_gain, log_scale, logit_bias):
    pairs, width = image_emb.shape
    tokens = text_tokens.shape[0]
    total_pairs = pairs * lax.axis_size(DP)
    plane, depth = lax.axis_size(PLANE), lax.axis_size(Z)
    wide = width + LANES
    ids = caption_ids[None, :]
    row, unit_image, image_norm, pooled, spill, tile, gain = local(
        prepare, [HBM] * 5,
        ((pairs, wide), BF16), ((pairs, width), F32), ((pairs, 1), F32), ((pairs, width), F32),
        ((1, width), F32), ((pairs, LANES), BF16), ((1, width), F32),
        scratch=(
            pltpu.SMEM((pairs,), jnp.int32), pltpu.VMEM((1, tokens), jnp.int32),
            pltpu.VMEM((pairs, width), BF16), pltpu.VMEM((tokens, width), BF16), pltpu.VMEM((width,), F32),
            pltpu.SemaphoreType.DMA((5,)),
        ),
    )(
        *(
            pltpu.with_memory_space_constraint(a, pltpu.HBM)
            for a in (groups, ids, image_emb, text_tokens, text_gain)
        )
    )

    arrived = from_behind(spill, -1)
    near = [row]
    for step in FROM[1:4]:
        near.append(exchange(row, Z, step))
    near = jnp.concatenate(near, axis=0)
    near = jnp.concatenate([near, exchange(near, Z, 1)], axis=0)
    rows, unit_text, text_norm = local(
        text_rows, [VMEM] * 4,
        ((plane, pairs, wide), BF16), ((pairs, width), F32), ((pairs, 1), F32),
    )(tile, pooled, arrived, gain)
    texts = to_all(rows, PLANE).reshape(plane * pairs, wide)

    far = exchange(near, C, 1)
    far, log_scale, logit_bias = lax.optimization_barrier((far, log_scale, logit_bias))
    lane = lax.broadcasted_iota(jnp.int32, (1, LANES), 1)
    knobs = jnp.where(lane == 0, log_scale[0], logit_bias[0])
    text_part, keep, send = local(
        pair_math, [VMEM] * 5,
        ((plane * pairs, wide + LANES), BF16), ((depth * pairs, width), F32), ((depth * pairs, width), BF16),
    )(knobs, near, far, texts, gain)

    back = to_all(text_part.reshape(plane, pairs, wide + LANES), PLANE)
    came = exchange(send, C, 1)
    pooled_grad, last, totals = local(
        text_gradient, [VMEM, VMEM, VMEM, VMEM],
        ((pairs, width), F32), ((1, width), F32), ((pairs, 2 * LANES), F32),
    )(back, unit_text, text_norm, gain)
    other = exchange(totals, C, 1)
    (blocks,) = local(pack, [SMEM] + [VMEM] * 4, ((depth, pairs, width + 4 * LANES), BF16))(
        lax.axis_index(Z)[None], keep, came, totals, other
    )
    line_back = to_all(blocks, Z)
    behind = from_behind(last, 1)
    (token_grad,) = local(token_rows, [VMEM] * 3, ((tokens, width), F32))(ids, pooled_grad, behind)
    image_grad, gain_grad, scalars = local(
        functools.partial(finish, count=float(total_pairs * total_pairs)), [VMEM] * 3,
        ((pairs, width), F32), ((width,), F32), ((3,), F32),
    )(line_back, unit_image, image_norm)
    return (image_grad, token_grad, gain_grad, scalars)


def solution(mesh):
    finer = Mesh(mesh.devices.reshape(4, 4, 8, 2), DP)
    placed = (P(DP, None), P(DP, None), P(DP), P(DP), P(), P(), P())
    return jax.shard_map(
        per_device,
        mesh=finer,
        in_specs=placed,
        out_specs=(P(DP, None), P(DP, None), P(), P()),
        check_vma=False,
    )
```

```python
import functools

import jax
import jax.numpy as jnp
from jax import lax
from jax.experimental import pallas as pl
from jax.experimental.pallas import tpu as pltpu
from jax.sharding import Mesh
from jax.sharding import PartitionSpec as P

Y, X, Z, C = ("dp_0", "dp_1", "dp_2", "dp_3")
DP = (Y, X, Z, C)
PLANE = (Y, X)
LANES = 128
F32, BF16 = jnp.float32, jnp.bfloat16
VMEM = pl.BlockSpec(memory_space=pltpu.VMEM)
SMEM = pl.BlockSpec(memory_space=pltpu.SMEM)
HBM = pl.BlockSpec(memory_space=pltpu.HBM)

FROM = (0, 2, 4, 6, 1, 3, 5, 7)


def from_behind(value, by):
    count = lax.axis_size(DP)
    pairs = [(i, i + by) for i in range(count) if 0 <= i + by < count]
    return lax.ppermute(value, DP, pairs)


def exchange(value, axis, bit):
    return lax.ppermute(value, axis, [(i, i ^ bit) for i in range(lax.axis_size(axis))])


def to_all(blocks, axes):
    count = lax.axis_size(axes)
    backward = [list(range(count))[::-1]]
    return lax.all_to_all(blocks, axes, 0, 0, tiled=True, axis_index_groups=backward)


def members(ids, pairs, copies):
    slot = lax.broadcasted_iota(jnp.int32, (2 * pairs * copies, 1), 0) % (2 * pairs)
    last = ids[:, ids.shape[1] - 1 :]
    wanted = jnp.where(slot < pairs, slot - (pairs - 1), jnp.where(slot == pairs, -pairs, 1))
    return (ids - last == wanted).astype(F32).astype(BF16)


def id_tile(groups_ref, pairs, for_text):
    row = lax.broadcasted_iota(jnp.int32, (pairs, LANES), 0)
    lane = lax.broadcasted_iota(jnp.int32, (pairs, LANES), 1)
    ids = jnp.zeros((pairs, LANES), jnp.int32)
    for r in range(pairs):
        ids = jnp.where(row == r, groups_ref[r], ids)
    high, low = (ids >> 8) << 8, ids & 255
    if for_text:
        cells = jnp.where(lane < 2, 1, jnp.where(lane == 2, -high, jnp.where(lane == 3, -low, 0)))
    else:
        cells = jnp.where(lane == 0, high, jnp.where(lane == 1, low, jnp.where(lane < 4, 1, 0)))
    return cells.astype(F32).astype(BF16)


def prepare(
    groups_hbm, ids_hbm, image_hbm, tokens_hbm, gain_hbm,
    row_ref, unit_ref, norm_ref, pooled_ref, spill_ref, tile_ref, gain_out,
    groups_ref, ids_ref, image_ref, tokens_ref, gain_ref, sems,
):
    pairs, width = image_hbm.shape
    moves = [
        pltpu.make_async_copy(source, target, sems.at[i])
        for i, (source, target) in enumerate(
            (
                (image_hbm, image_ref), (groups_hbm, groups_ref), (ids_hbm, ids_ref),
                (tokens_hbm, tokens_ref), (gain_hbm, gain_ref),
            )
        )
    ]
    for move in moves:
        move.start()
    moves[0].wait()
    moves[1].wait()
    image = image_ref[...].astype(F32)
    norm = jnp.sqrt(jnp.sum(image * image, axis=1, keepdims=True))
    unit = image / norm
    unit_ref[...] = unit
    norm_ref[...] = norm
    row_ref[:, :width] = unit.astype(BF16)
    row_ref[:, width:] = id_tile(groups_ref, pairs, False)
    tile_ref[...] = id_tile(groups_ref, pairs, True)
    moves[4].wait()
    gain_out[...] = gain_ref[...][None, :]
    moves[2].wait()
    moves[3].wait()
    sums = jnp.dot(members(ids_ref[...], pairs, 1), tokens_ref[...], preferred_element_type=F32)
    pooled_ref[...] = sums[:pairs]
    spill_ref[...] = sums[pairs : pairs + 1]


def text_rows(tile_ref, pooled_ref, arrived_ref, gain_ref, rows_ref, unit_ref, norm_ref):
    pairs, width = pooled_ref.shape
    last = lax.broadcasted_iota(jnp.int32, (pairs, 1), 0) == pairs - 1
    pooled = pooled_ref[...] + jnp.where(last, arrived_ref[...], 0.0)
    embedded = pooled * gain_ref[...]
    norm = jnp.sqrt(jnp.sum(embedded * embedded, axis=1, keepdims=True))
    unit = embedded / norm
    unit_ref[...] = unit
    norm_ref[...] = norm
    low, ids = unit.astype(BF16), tile_ref[...]
    for k in range(rows_ref.shape[0]):
        rows_ref[k, :, :width] = low
        rows_ref[k, :, width:] = ids


def pair_math(knobs_ref, near_ref, far_ref, text_ref, gain_ref, text_out, keep_out, send_out):
    width = gain_ref.shape[1]
    scale = jnp.exp(knobs_ref[:, :1])
    rows = jnp.concatenate([near_ref[...], far_ref[...]], axis=0)
    image, text = rows[:, :width], text_ref[:, :width]
    contract = (((1,), (1,)), ((), ()))
    scaled = scale * lax.dot_general(image, text, contract, preferred_element_type=F32)
    apart = lax.dot_general(
        rows[:, width:], text_ref[:, width:], contract, preferred_element_type=F32
    )
    match = apart == 0.0
    logits = scaled + knobs_ref[:, 1:2]
    margin = jnp.where(match, -logits, logits)
    tail = jnp.exp(-jnp.abs(margin))
    losses = jnp.maximum(margin, 0.0) + jnp.log1p(tail)
    sigmoid = jnp.where(margin >= 0.0, 1.0, tail) / (1.0 + tail)
    coeffs = jnp.where(match, -sigmoid, sigmoid)
    image_part = scale * jnp.dot(coeffs.astype(BF16), text, preferred_element_type=F32)
    text_part = scale * jnp.dot(coeffs.T.astype(BF16), image, preferred_element_type=F32)
    half = keep_out.shape[0]
    keep_out[...] = image_part[:half]
    send_out[...] = image_part[half:].astype(BF16)
    text_out[:, :width] = text_part.astype(BF16)

    unit = text.astype(F32)
    along = jnp.sum(unit * text_part, axis=1, keepdims=True)
    gain_terms = jnp.sum((text_part - unit * along) * unit, axis=0, keepdims=True) / gain_ref[...]
    row = lax.broadcasted_iota(jnp.int32, (8, LANES), 0)
    lane = lax.broadcasted_iota(jnp.int32, (8, LANES), 1)
    first = jnp.zeros((8, LANES), F32)
    for r in range(8):
        first = jnp.where(row == r, gain_terms[:, LANES * r : LANES * (r + 1)], first)
    second = jnp.where(row == 0, gain_terms[:, 8 * LANES : 9 * LANES], 0.0)
    for i, terms in enumerate((losses, coeffs * scaled, coeffs)):
        total = jnp.sum(jnp.sum(terms, axis=0, keepdims=True), axis=1, keepdims=True)
        high = total.astype(BF16).astype(F32)
        second = jnp.where((row == 1) & (lane == i), high, second)
        second = jnp.where((row == 2) & (lane == i), total - high, second)
    packed = jnp.concatenate([first, second], axis=1).astype(BF16)
    for k in range(text_out.shape[0] // 8):
        text_out[8 * k : 8 * (k + 1), width:] = packed


def text_gradient(back_ref, unit_ref, norm_ref, gain_ref, grad_out, last_out, totals_out):
    pairs, width = unit_ref.shape
    total = jnp.sum(back_ref[...].astype(F32), axis=0)
    totals_out[...] = total[:, width:]
    grad, unit = total[:, :width], unit_ref[...]
    grad = grad - unit * jnp.sum(unit * grad, axis=1, keepdims=True)
    grad = grad / norm_ref[...] * gain_ref[...]
    grad_out[...] = grad
    last_out[...] = grad[pairs - 1 :]


def pack(place_ref, keep_ref, came_ref, totals_ref, other_ref, out_ref):
    places, pairs, _ = out_ref.shape
    width = keep_ref.shape[1]
    total = totals_ref[...] + other_ref[...]
    high = total.astype(BF16)
    low = (total - high.astype(F32)).astype(BF16)
    for k in range(places):
        rows = slice(pairs * k, pairs * (k + 1))
        block = keep_ref[rows] + came_ref[rows].astype(F32)
        place = places - 1 - (place_ref[0] ^ FROM[k])
        out_ref[place, :, :width] = block.astype(BF16)
        out_ref[place, :, width : width + 2 * LANES] = high
        out_ref[place, :, width + 2 * LANES :] = low


def token_rows(ids_ref, grad_ref, behind_ref, token_out):
    pairs, width = grad_ref.shape
    table = jnp.concatenate(
        [grad_ref[...], jnp.broadcast_to(behind_ref[...], (pairs, width))], axis=0
    )
    high = table.astype(BF16)
    low = (table - high.astype(F32)).astype(BF16)
    token_out[...] = lax.dot_general(
        members(ids_ref[...], pairs, 2),
        jnp.concatenate([high, low], axis=0),
        (((0,), (0,)), ((), ())),
        preferred_element_type=F32,
    )


def finish(back_ref, unit_ref, norm_ref, image_out, gain_out, scalars_out, *, count):
    width = unit_ref.shape[1]
    total = jnp.sum(back_ref[...].astype(F32), axis=0)
    first = total[:, width : width + LANES] + total[:, width + 2 * LANES : width + 3 * LANES]
    second = total[:, width + LANES : width + 2 * LANES] + total[:, width + 3 * LANES :]
    gain_out[...] = jnp.concatenate([first[r] for r in range(8)] + [second[0]])
    scalars_out[...] = ((second[1] + second[2]) / count)[:3]
    grad, unit = total[:, :width], unit_ref[...]
    grad = grad - unit * jnp.sum(unit * grad, axis=1, keepdims=True)
    image_out[...] = grad / norm_ref[...]


def local(kernel, specs, *outs, scratch=()):
    return pl.pallas_call(
        kernel,
        in_specs=specs,
        out_specs=[VMEM] * len(outs),
        out_shape=[jax.ShapeDtypeStruct(*o) for o in outs],
        scratch_shapes=scratch,
        compiler_params=pltpu.CompilerParams(vmem_limit_bytes=16 << 20),
    )


def per_device(image_emb, text_tokens, caption_ids, groups, text_gain, log_scale, logit_bias):
    pairs, width = image_emb.shape
    tokens = text_tokens.shape[0]
    total_pairs = pairs * lax.axis_size(DP)
    plane, depth = lax.axis_size(PLANE), lax.axis_size(Z)
    wide = width + LANES
    ids = caption_ids[None, :]
    row, unit_image, image_norm, pooled, spill, tile, gain = local(
        prepare, [HBM] * 5,
        ((pairs, wide), BF16), ((pairs, width), F32), ((pairs, 1), F32), ((pairs, width), F32),
        ((1, width), F32), ((pairs, LANES), BF16), ((1, width), F32),
        scratch=(
            pltpu.SMEM((pairs,), jnp.int32), pltpu.VMEM((1, tokens), jnp.int32),
            pltpu.VMEM((pairs, width), BF16), pltpu.VMEM((tokens, width), BF16), pltpu.VMEM((width,), F32),
            pltpu.SemaphoreType.DMA((5,)),
        ),
    )(
        *(
            pltpu.with_memory_space_constraint(a, pltpu.HBM)
            for a in (groups, ids, image_emb, text_tokens, text_gain)
        )
    )

    arrived = from_behind(spill, -1)
    near = [row]
    for step in FROM[1:4]:
        near.append(exchange(row, Z, step))
    near = jnp.concatenate(near, axis=0)
    near = jnp.concatenate([near, exchange(near, Z, 1)], axis=0)
    rows, unit_text, text_norm = local(
        text_rows, [VMEM] * 4,
        ((plane, pairs, wide), BF16), ((pairs, width), F32), ((pairs, 1), F32),
    )(tile, pooled, arrived, gain)
    texts = to_all(rows, PLANE).reshape(plane * pairs, wide)

    far = exchange(near, C, 1)
    far, log_scale, logit_bias = lax.optimization_barrier((far, log_scale, logit_bias))
    lane = lax.broadcasted_iota(jnp.int32, (1, LANES), 1)
    knobs = jnp.where(lane == 0, log_scale[0], logit_bias[0])
    text_part, keep, send = local(
        pair_math, [VMEM] * 5,
        ((plane * pairs, wide + LANES), BF16), ((depth * pairs, width), F32), ((depth * pairs, width), BF16),
    )(knobs, near, far, texts, gain)

    back = to_all(text_part.reshape(plane, pairs, wide + LANES), PLANE)
    came = exchange(send, C, 1)
    pooled_grad, last, totals = local(
        text_gradient, [VMEM, VMEM, VMEM, VMEM],
        ((pairs, width), F32), ((1, width), F32), ((pairs, 2 * LANES), F32),
    )(back, unit_text, text_norm, gain)
    other = exchange(totals, C, 1)
    (blocks,) = local(pack, [SMEM] + [VMEM] * 4, ((depth, pairs, width + 4 * LANES), BF16))(
        lax.axis_index(Z)[None], keep, came, totals, other
    )
    line_back = to_all(blocks, Z)
    behind = from_behind(last, 1)
    (token_grad,) = local(token_rows, [VMEM] * 3, ((tokens, width), F32))(ids, pooled_grad, behind)
    image_grad, gain_grad, scalars = local(
        functools.partial(finish, count=float(total_pairs * total_pairs)), [VMEM] * 3,
        ((pairs, width), F32), ((width,), F32), ((3,), F32),
    )(line_back, unit_image, image_norm)
    return (image_grad, token_grad, gain_grad, scalars)


def solution(mesh):
    finer = Mesh(mesh.devices.reshape(4, 4, 8, 2), DP)
    placed = (P(DP, None), P(DP, None), P(DP), P(DP), P(), P(), P())
    return jax.shard_map(
        per_device,
        mesh=finer,
        in_specs=placed,
        out_specs=(P(DP, None), P(DP, None), P(), P()),
        check_vma=False,
    )
```

```python
import functools

import jax
import jax.numpy as jnp
from jax import lax
from jax.experimental import pallas as pl
from jax.experimental.pallas import tpu as pltpu
from jax.sharding import Mesh
from jax.sharding import PartitionSpec as P

Y, X, Z, C = ("dp_0", "dp_1", "dp_2", "dp_3")
DP = (Y, X, Z, C)
PLANE = (Y, X)
LANES = 128
F32, BF16 = jnp.float32, jnp.bfloat16
VMEM = pl.BlockSpec(memory_space=pltpu.VMEM)
SMEM = pl.BlockSpec(memory_space=pltpu.SMEM)
HBM = pl.BlockSpec(memory_space=pltpu.HBM)

FROM = (0, 2, 4, 6, 1, 3, 5, 7)


def from_beside(value, by):
    count, parts = lax.axis_size(DP), []
    for within in (False, True):
        pairs = [
            (i, i + by) for i in range(count) if 0 <= i + by < count and (i // 2 == (i + by) // 2) == within
        ]
        parts.append(lax.ppermute(value, DP, pairs))
    return parts


def exchange(value, axis, bit):
    return lax.ppermute(value, axis, [(i, i ^ bit) for i in range(lax.axis_size(axis))])


def to_all(blocks, axes):
    count = lax.axis_size(axes)
    backward = [list(range(count))[::-1]]
    return lax.all_to_all(blocks, axes, 0, 0, tiled=True, axis_index_groups=backward)


def members(ids, pairs, copies):
    slot = lax.broadcasted_iota(jnp.int32, (2 * pairs * copies, 1), 0) % (2 * pairs)
    last = ids[:, ids.shape[1] - 1 :]
    wanted = jnp.where(slot < pairs, slot - (pairs - 1), jnp.where(slot == pairs, -pairs, 1))
    return (ids - last == wanted).astype(F32).astype(BF16)


def id_tile(groups_ref, pairs, for_text):
    row = lax.broadcasted_iota(jnp.int32, (pairs, LANES), 0)
    lane = lax.broadcasted_iota(jnp.int32, (pairs, LANES), 1)
    ids = jnp.zeros((pairs, LANES), jnp.int32)
    for r in range(pairs):
        ids = jnp.where(row == r, groups_ref[r], ids)
    high, low = (ids >> 8) << 8, ids & 255
    if for_text:
        cells = jnp.where(lane < 2, 1, jnp.where(lane == 2, -high, jnp.where(lane == 3, -low, 0)))
    else:
        cells = jnp.where(lane == 0, high, jnp.where(lane == 1, low, jnp.where(lane < 4, 1, 0)))
    return cells.astype(F32).astype(BF16)


def prepare(
    groups_hbm, ids_hbm, image_hbm, tokens_hbm, gain_hbm,
    row_ref, unit_ref, norm_ref, pooled_ref, spill_ref, tile_ref, gain_out,
    groups_ref, ids_ref, image_ref, tokens_ref, gain_ref, sems,
):
    pairs, width = image_hbm.shape
    moves = [
        pltpu.make_async_copy(source, target, sems.at[i])
        for i, (source, target) in enumerate(
            (
                (image_hbm, image_ref), (groups_hbm, groups_ref), (ids_hbm, ids_ref),
                (tokens_hbm, tokens_ref), (gain_hbm, gain_ref),
            )
        )
    ]
    for move in moves:
        move.start()
    moves[0].wait()
    moves[1].wait()
    image = image_ref[...].astype(F32)
    norm = jnp.sqrt(jnp.sum(image * image, axis=1, keepdims=True))
    unit = image / norm
    unit_ref[...] = unit
    norm_ref[...] = norm
    row_ref[:, :width] = unit.astype(BF16)
    row_ref[:, width:] = id_tile(groups_ref, pairs, False)
    tile_ref[...] = id_tile(groups_ref, pairs, True)
    moves[4].wait()
    gain_out[...] = gain_ref[...][None, :]
    moves[2].wait()
    moves[3].wait()
    sums = jnp.dot(members(ids_ref[...], pairs, 1), tokens_ref[...], preferred_element_type=F32)
    pooled_ref[...] = sums[:pairs]
    spill_ref[...] = sums[pairs : pairs + 1]


def text_rows(tile_ref, pooled_ref, chip_ref, core_ref, gain_ref, rows_ref, unit_ref, norm_ref):
    pairs, width = pooled_ref.shape
    last = lax.broadcasted_iota(jnp.int32, (pairs, 1), 0) == pairs - 1
    pooled = pooled_ref[...] + jnp.where(last, chip_ref[...] + core_ref[...], 0.0)
    embedded = pooled * gain_ref[...]
    norm = jnp.sqrt(jnp.sum(embedded * embedded, axis=1, keepdims=True))
    unit = embedded / norm
    unit_ref[...] = unit
    norm_ref[...] = norm
    low, ids = unit.astype(BF16), tile_ref[...]
    for k in range(rows_ref.shape[0]):
        rows_ref[k, :, :width] = low
        rows_ref[k, :, width:] = ids


def pair_math(knobs_ref, near_ref, far_ref, text_ref, gain_ref, text_out, keep_out, send_out):
    width = gain_ref.shape[1]
    scale = jnp.exp(knobs_ref[:, :1])
    rows = jnp.concatenate([near_ref[...], far_ref[...]], axis=0)
    image, text = rows[:, :width], text_ref[:, :width]
    contract = (((1,), (1,)), ((), ()))
    scaled = scale * lax.dot_general(image, text, contract, preferred_element_type=F32)
    apart = lax.dot_general(
        rows[:, width:], text_ref[:, width:], contract, preferred_element_type=F32
    )
    match = apart == 0.0
    logits = scaled + knobs_ref[:, 1:2]
    margin = jnp.where(match, -logits, logits)
    tail = jnp.exp(-jnp.abs(margin))
    losses = jnp.maximum(margin, 0.0) + jnp.log1p(tail)
    sigmoid = jnp.where(margin >= 0.0, 1.0, tail) / (1.0 + tail)
    coeffs = jnp.where(match, -sigmoid, sigmoid)
    image_part = scale * jnp.dot(coeffs.astype(BF16), text, preferred_element_type=F32)
    text_part = scale * jnp.dot(coeffs.T.astype(BF16), image, preferred_element_type=F32)
    half = keep_out.shape[0]
    keep_out[...] = image_part[:half]
    send_out[...] = image_part[half:].astype(BF16)
    text_out[:, :width] = text_part.astype(BF16)

    unit = text.astype(F32)
    along = jnp.sum(unit * text_part, axis=1, keepdims=True)
    gain_terms = jnp.sum((text_part - unit * along) * unit, axis=0, keepdims=True) / gain_ref[...]
    row = lax.broadcasted_iota(jnp.int32, (8, LANES), 0)
    lane = lax.broadcasted_iota(jnp.int32, (8, LANES), 1)
    first = jnp.zeros((8, LANES), F32)
    for r in range(8):
        first = jnp.where(row == r, gain_terms[:, LANES * r : LANES * (r + 1)], first)
    second = jnp.where(row == 0, gain_terms[:, 8 * LANES : 9 * LANES], 0.0)
    for i, terms in enumerate((losses, coeffs * scaled, coeffs)):
        total = jnp.sum(jnp.sum(terms, axis=0, keepdims=True), axis=1, keepdims=True)
        high = total.astype(BF16).astype(F32)
        second = jnp.where((row == 1) & (lane == i), high, second)
        second = jnp.where((row == 2) & (lane == i), total - high, second)
    packed = jnp.concatenate([first, second], axis=1).astype(BF16)
    for k in range(text_out.shape[0] // 8):
        text_out[8 * k : 8 * (k + 1), width:] = packed


def text_gradient(back_ref, unit_ref, norm_ref, gain_ref, grad_out, last_out, totals_out):
    pairs, width = unit_ref.shape
    total = jnp.sum(back_ref[...].astype(F32), axis=0)
    totals_out[...] = total[:, width:]
    grad, unit = total[:, :width], unit_ref[...]
    grad = grad - unit * jnp.sum(unit * grad, axis=1, keepdims=True)
    grad = grad / norm_ref[...] * gain_ref[...]
    grad_out[...] = grad
    last_out[...] = grad[pairs - 1 :]


def pack(place_ref, keep_ref, came_ref, totals_ref, other_ref, out_ref):
    places, pairs, _ = out_ref.shape
    width = keep_ref.shape[1]
    total = totals_ref[...] + other_ref[...]
    high = total.astype(BF16)
    low = (total - high.astype(F32)).astype(BF16)
    for k in range(places):
        rows = slice(pairs * k, pairs * (k + 1))
        block = keep_ref[rows] + came_ref[rows].astype(F32)
        place = places - 1 - (place_ref[0] ^ FROM[k])
        out_ref[place, :, :width] = block.astype(BF16)
        out_ref[place, :, width : width + 2 * LANES] = high
        out_ref[place, :, width + 2 * LANES :] = low


def token_rows(ids_ref, grad_ref, chip_ref, core_ref, token_out):
    pairs, width = grad_ref.shape
    table = jnp.concatenate(
        [grad_ref[...], jnp.broadcast_to(chip_ref[...] + core_ref[...], (pairs, width))], axis=0
    )
    high = table.astype(BF16)
    low = (table - high.astype(F32)).astype(BF16)
    token_out[...] = lax.dot_general(
        members(ids_ref[...], pairs, 2),
        jnp.concatenate([high, low], axis=0),
        (((0,), (0,)), ((), ())),
        preferred_element_type=F32,
    )


def finish(back_ref, unit_ref, norm_ref, image_out, gain_out, scalars_out, *, count):
    width = unit_ref.shape[1]
    total = jnp.sum(back_ref[...].astype(F32), axis=0)
    first = total[:, width : width + LANES] + total[:, width + 2 * LANES : width + 3 * LANES]
    second = total[:, width + LANES : width + 2 * LANES] + total[:, width + 3 * LANES :]
    gain_out[...] = jnp.concatenate([first[r] for r in range(8)] + [second[0]])
    scalars_out[...] = ((second[1] + second[2]) / count)[:3]
    grad, unit = total[:, :width], unit_ref[...]
    grad = grad - unit * jnp.sum(unit * grad, axis=1, keepdims=True)
    image_out[...] = grad / norm_ref[...]


def local(kernel, specs, *outs, scratch=()):
    return pl.pallas_call(
        kernel,
        in_specs=specs,
        out_specs=[VMEM] * len(outs),
        out_shape=[jax.ShapeDtypeStruct(*o) for o in outs],
        scratch_shapes=scratch,
        compiler_params=pltpu.CompilerParams(vmem_limit_bytes=16 << 20),
    )


def per_device(image_emb, text_tokens, caption_ids, groups, text_gain, log_scale, logit_bias):
    pairs, width = image_emb.shape
    tokens = text_tokens.shape[0]
    total_pairs = pairs * lax.axis_size(DP)
    plane, depth = lax.axis_size(PLANE), lax.axis_size(Z)
    wide = width + LANES
    ids = caption_ids[None, :]
    row, unit_image, image_norm, pooled, spill, tile, gain = local(
        prepare, [HBM] * 5,
        ((pairs, wide), BF16), ((pairs, width), F32), ((pairs, 1), F32), ((pairs, width), F32),
        ((1, width), F32), ((pairs, LANES), BF16), ((1, width), F32),
        scratch=(
            pltpu.SMEM((pairs,), jnp.int32), pltpu.VMEM((1, tokens), jnp.int32),
            pltpu.VMEM((pairs, width), BF16), pltpu.VMEM((tokens, width), BF16), pltpu.VMEM((width,), F32),
            pltpu.SemaphoreType.DMA((5,)),
        ),
    )(
        *(
            pltpu.with_memory_space_constraint(a, pltpu.HBM)
            for a in (groups, ids, image_emb, text_tokens, text_gain)
        )
    )

    arrived = from_beside(spill, -1)
    near = [row]
    for step in FROM[1:4]:
        near.append(exchange(row, Z, step))
    near = jnp.concatenate(near, axis=0)
    near = jnp.concatenate([near, exchange(near, Z, 1)], axis=0)
    rows, unit_text, text_norm = local(
        text_rows, [VMEM] * 5,
        ((plane, pairs, wide), BF16), ((pairs, width), F32), ((pairs, 1), F32),
    )(tile, pooled, *arrived, gain)
    texts = to_all(rows, PLANE).reshape(plane * pairs, wide)

    far = exchange(near, C, 1)
    far, log_scale, logit_bias = lax.optimization_barrier((far, log_scale, logit_bias))
    lane = lax.broadcasted_iota(jnp.int32, (1, LANES), 1)
    knobs = jnp.where(lane == 0, log_scale[0], logit_bias[0])
    text_part, keep, send = local(
        pair_math, [VMEM] * 5,
        ((plane * pairs, wide + LANES), BF16), ((depth * pairs, width), F32), ((depth * pairs, width), BF16),
    )(knobs, near, far, texts, gain)

    back = to_all(text_part.reshape(plane, pairs, wide + LANES), PLANE)
    came = exchange(send, C, 1)
    pooled_grad, last, totals = local(
        text_gradient, [VMEM, VMEM, VMEM, VMEM],
        ((pairs, width), F32), ((1, width), F32), ((pairs, 2 * LANES), F32),
    )(back, unit_text, text_norm, gain)
    other = exchange(totals, C, 1)
    (blocks,) = local(pack, [SMEM] + [VMEM] * 4, ((depth, pairs, width + 4 * LANES), BF16))(
        lax.axis_index(Z)[None], keep, came, totals, other
    )
    line_back = to_all(blocks, Z)
    behind = from_beside(last, 1)
    (token_grad,) = local(token_rows, [VMEM] * 4, ((tokens, width), F32))(ids, pooled_grad, *behind)
    image_grad, gain_grad, scalars = local(
        functools.partial(finish, count=float(total_pairs * total_pairs)), [VMEM] * 3,
        ((pairs, width), F32), ((width,), F32), ((3,), F32),
    )(line_back, unit_image, image_norm)
    return (image_grad, token_grad, gain_grad, scalars)


def solution(mesh):
    finer = Mesh(mesh.devices.reshape(4, 4, 8, 2), DP)
    placed = (P(DP, None), P(DP, None), P(DP), P(DP), P(), P(), P())
    return jax.shard_map(
        per_device,
        mesh=finer,
        in_specs=placed,
        out_specs=(P(DP, None), P(DP, None), P(), P()),
        check_vma=False,
    )
```

```python
import functools

import jax
import jax.numpy as jnp
from jax import lax
from jax.experimental import pallas as pl
from jax.experimental.pallas import tpu as pltpu
from jax.sharding import Mesh
from jax.sharding import PartitionSpec as P

Y, X, Z, C = ("dp_0", "dp_1", "dp_2", "dp_3")
DP = (Y, X, Z, C)
PLANE = (Y, X)
LANES = 128
F32, BF16 = jnp.float32, jnp.bfloat16
VMEM = pl.BlockSpec(memory_space=pltpu.VMEM)
SMEM = pl.BlockSpec(memory_space=pltpu.SMEM)
HBM = pl.BlockSpec(memory_space=pltpu.HBM)

FROM = (0, 2, 4, 6, 1, 3, 5, 7)


def from_beside(value, by):
    count = lax.axis_size(DP)
    return lax.ppermute(value, DP, [(i, (i + by) % count) for i in range(count)])


def exchange(value, axis, bit):
    return lax.ppermute(value, axis, [(i, i ^ bit) for i in range(lax.axis_size(axis))])


def to_all(blocks, axes):
    count = lax.axis_size(axes)
    backward = [list(range(count))[::-1]]
    return lax.all_to_all(blocks, axes, 0, 0, tiled=True, axis_index_groups=backward)


def members(ids, pairs, copies):
    slot = lax.broadcasted_iota(jnp.int32, (2 * pairs * copies, 1), 0) % (2 * pairs)
    last = ids[:, ids.shape[1] - 1 :]
    wanted = jnp.where(slot < pairs, slot - (pairs - 1), jnp.where(slot == pairs, -pairs, 1))
    return (ids - last == wanted).astype(F32).astype(BF16)


def id_tile(groups_ref, pairs, for_text):
    row = lax.broadcasted_iota(jnp.int32, (pairs, LANES), 0)
    lane = lax.broadcasted_iota(jnp.int32, (pairs, LANES), 1)
    ids = jnp.zeros((pairs, LANES), jnp.int32)
    for r in range(pairs):
        ids = jnp.where(row == r, groups_ref[r], ids)
    high, low = (ids >> 8) << 8, ids & 255
    if for_text:
        cells = jnp.where(lane < 2, 1, jnp.where(lane == 2, -high, jnp.where(lane == 3, -low, 0)))
    else:
        cells = jnp.where(lane == 0, high, jnp.where(lane == 1, low, jnp.where(lane < 4, 1, 0)))
    return cells.astype(F32).astype(BF16)


def prepare(
    groups_hbm, ids_hbm, image_hbm, tokens_hbm, gain_hbm,
    row_ref, unit_ref, norm_ref, pooled_ref, spill_ref, tile_ref, gain_out,
    groups_ref, ids_ref, image_ref, tokens_ref, gain_ref, sems,
):
    pairs, width = image_hbm.shape
    moves = [
        pltpu.make_async_copy(source, target, sems.at[i])
        for i, (source, target) in enumerate(
            (
                (image_hbm, image_ref), (groups_hbm, groups_ref), (ids_hbm, ids_ref),
                (tokens_hbm, tokens_ref), (gain_hbm, gain_ref),
            )
        )
    ]
    for move in moves:
        move.start()
    moves[0].wait()
    moves[1].wait()
    image = image_ref[...].astype(F32)
    norm = jnp.sqrt(jnp.sum(image * image, axis=1, keepdims=True))
    unit = image / norm
    unit_ref[...] = unit
    norm_ref[...] = norm
    row_ref[:, :width] = unit.astype(BF16)
    row_ref[:, width:] = id_tile(groups_ref, pairs, False)
    tile_ref[...] = id_tile(groups_ref, pairs, True)
    moves[4].wait()
    gain_out[...] = gain_ref[...][None, :]
    moves[2].wait()
    moves[3].wait()
    sums = jnp.dot(members(ids_ref[...], pairs, 1), tokens_ref[...], preferred_element_type=F32)
    pooled_ref[...] = sums[:pairs]
    spill_ref[...] = sums[pairs : pairs + 1]


def text_rows(tile_ref, pooled_ref, arrived_ref, gain_ref, rows_ref, unit_ref, norm_ref):
    pairs, width = pooled_ref.shape
    last = lax.broadcasted_iota(jnp.int32, (pairs, 1), 0) == pairs - 1
    pooled = pooled_ref[...] + jnp.where(last, arrived_ref[...], 0.0)
    embedded = pooled * gain_ref[...]
    norm = jnp.sqrt(jnp.sum(embedded * embedded, axis=1, keepdims=True))
    unit = embedded / norm
    unit_ref[...] = unit
    norm_ref[...] = norm
    low, ids = unit.astype(BF16), tile_ref[...]
    for k in range(rows_ref.shape[0]):
        rows_ref[k, :, :width] = low
        rows_ref[k, :, width:] = ids


def pair_math(knobs_ref, near_ref, far_ref, text_ref, gain_ref, text_out, keep_out, send_out):
    width = gain_ref.shape[1]
    scale = jnp.exp(knobs_ref[:, :1])
    rows = jnp.concatenate([near_ref[...], far_ref[...]], axis=0)
    image, text = rows[:, :width], text_ref[:, :width]
    contract = (((1,), (1,)), ((), ()))
    scaled = scale * lax.dot_general(image, text, contract, preferred_element_type=F32)
    apart = lax.dot_general(
        rows[:, width:], text_ref[:, width:], contract, preferred_element_type=F32
    )
    match = apart == 0.0
    logits = scaled + knobs_ref[:, 1:2]
    margin = jnp.where(match, -logits, logits)
    tail = jnp.exp(-jnp.abs(margin))
    losses = jnp.maximum(margin, 0.0) + jnp.log1p(tail)
    sigmoid = jnp.where(margin >= 0.0, 1.0, tail) / (1.0 + tail)
    coeffs = jnp.where(match, -sigmoid, sigmoid)
    image_part = scale * jnp.dot(coeffs.astype(BF16), text, preferred_element_type=F32)
    text_part = scale * jnp.dot(coeffs.T.astype(BF16), image, preferred_element_type=F32)
    half = keep_out.shape[0]
    keep_out[...] = image_part[:half]
    send_out[...] = image_part[half:].astype(BF16)
    text_out[:, :width] = text_part.astype(BF16)

    unit = text.astype(F32)
    along = jnp.sum(unit * text_part, axis=1, keepdims=True)
    gain_terms = jnp.sum((text_part - unit * along) * unit, axis=0, keepdims=True) / gain_ref[...]
    row = lax.broadcasted_iota(jnp.int32, (8, LANES), 0)
    lane = lax.broadcasted_iota(jnp.int32, (8, LANES), 1)
    first = jnp.zeros((8, LANES), F32)
    for r in range(8):
        first = jnp.where(row == r, gain_terms[:, LANES * r : LANES * (r + 1)], first)
    second = jnp.where(row == 0, gain_terms[:, 8 * LANES : 9 * LANES], 0.0)
    for i, terms in enumerate((losses, coeffs * scaled, coeffs)):
        total = jnp.sum(jnp.sum(terms, axis=0, keepdims=True), axis=1, keepdims=True)
        high = total.astype(BF16).astype(F32)
        second = jnp.where((row == 1) & (lane == i), high, second)
        second = jnp.where((row == 2) & (lane == i), total - high, second)
    packed = jnp.concatenate([first, second], axis=1).astype(BF16)
    for k in range(text_out.shape[0] // 8):
        text_out[8 * k : 8 * (k + 1), width:] = packed


def text_gradient(back_ref, unit_ref, norm_ref, gain_ref, grad_out, last_out, totals_out):
    pairs, width = unit_ref.shape
    total = jnp.sum(back_ref[...].astype(F32), axis=0)
    totals_out[...] = total[:, width:]
    grad, unit = total[:, :width], unit_ref[...]
    grad = grad - unit * jnp.sum(unit * grad, axis=1, keepdims=True)
    grad = grad / norm_ref[...] * gain_ref[...]
    grad_out[...] = grad
    last_out[...] = grad[pairs - 1 :]


def pack(place_ref, keep_ref, came_ref, totals_ref, other_ref, out_ref):
    places, pairs, _ = out_ref.shape
    width = keep_ref.shape[1]
    total = totals_ref[...] + other_ref[...]
    high = total.astype(BF16)
    low = (total - high.astype(F32)).astype(BF16)
    for k in range(places):
        rows = slice(pairs * k, pairs * (k + 1))
        block = keep_ref[rows] + came_ref[rows].astype(F32)
        place = places - 1 - (place_ref[0] ^ FROM[k])
        out_ref[place, :, :width] = block.astype(BF16)
        out_ref[place, :, width : width + 2 * LANES] = high
        out_ref[place, :, width + 2 * LANES :] = low


def token_rows(ids_ref, grad_ref, behind_ref, token_out):
    pairs, width = grad_ref.shape
    table = jnp.concatenate(
        [grad_ref[...], jnp.broadcast_to(behind_ref[...], (pairs, width))], axis=0
    )
    high = table.astype(BF16)
    low = (table - high.astype(F32)).astype(BF16)
    token_out[...] = lax.dot_general(
        members(ids_ref[...], pairs, 2),
        jnp.concatenate([high, low], axis=0),
        (((0,), (0,)), ((), ())),
        preferred_element_type=F32,
    )


def finish(back_ref, unit_ref, norm_ref, image_out, gain_out, scalars_out, *, count):
    width = unit_ref.shape[1]
    total = jnp.sum(back_ref[...].astype(F32), axis=0)
    first = total[:, width : width + LANES] + total[:, width + 2 * LANES : width + 3 * LANES]
    second = total[:, width + LANES : width + 2 * LANES] + total[:, width + 3 * LANES :]
    gain_out[...] = jnp.concatenate([first[r] for r in range(8)] + [second[0]])
    scalars_out[...] = ((second[1] + second[2]) / count)[:3]
    grad, unit = total[:, :width], unit_ref[...]
    grad = grad - unit * jnp.sum(unit * grad, axis=1, keepdims=True)
    image_out[...] = grad / norm_ref[...]


def local(kernel, specs, *outs, scratch=()):
    return pl.pallas_call(
        kernel,
        in_specs=specs,
        out_specs=[VMEM] * len(outs),
        out_shape=[jax.ShapeDtypeStruct(*o) for o in outs],
        scratch_shapes=scratch,
        compiler_params=pltpu.CompilerParams(vmem_limit_bytes=16 << 20),
    )


def per_device(image_emb, text_tokens, caption_ids, groups, text_gain, log_scale, logit_bias):
    pairs, width = image_emb.shape
    tokens = text_tokens.shape[0]
    total_pairs = pairs * lax.axis_size(DP)
    plane, depth = lax.axis_size(PLANE), lax.axis_size(Z)
    wide = width + LANES
    ids = caption_ids[None, :]
    row, unit_image, image_norm, pooled, spill, tile, gain = local(
        prepare, [HBM] * 5,
        ((pairs, wide), BF16), ((pairs, width), F32), ((pairs, 1), F32), ((pairs, width), F32),
        ((1, width), F32), ((pairs, LANES), BF16), ((1, width), F32),
        scratch=(
            pltpu.SMEM((pairs,), jnp.int32), pltpu.VMEM((1, tokens), jnp.int32),
            pltpu.VMEM((pairs, width), BF16), pltpu.VMEM((tokens, width), BF16), pltpu.VMEM((width,), F32),
            pltpu.SemaphoreType.DMA((5,)),
        ),
    )(
        *(
            pltpu.with_memory_space_constraint(a, pltpu.HBM)
            for a in (groups, ids, image_emb, text_tokens, text_gain)
        )
    )

    arrived = from_beside(spill, -1)
    near = [row]
    for step in FROM[1:4]:
        near.append(exchange(row, Z, step))
    near = jnp.concatenate(near, axis=0)
    near = jnp.concatenate([near, exchange(near, Z, 1)], axis=0)
    rows, unit_text, text_norm = local(
        text_rows, [VMEM] * 4,
        ((plane, pairs, wide), BF16), ((pairs, width), F32), ((pairs, 1), F32),
    )(tile, pooled, arrived, gain)
    texts = to_all(rows, PLANE).reshape(plane * pairs, wide)

    far = exchange(near, C, 1)
    far, log_scale, logit_bias = lax.optimization_barrier((far, log_scale, logit_bias))
    lane = lax.broadcasted_iota(jnp.int32, (1, LANES), 1)
    knobs = jnp.where(lane == 0, log_scale[0], logit_bias[0])
    text_part, keep, send = local(
        pair_math, [VMEM] * 5,
        ((plane * pairs, wide + LANES), BF16), ((depth * pairs, width), F32), ((depth * pairs, width), BF16),
    )(knobs, near, far, texts, gain)

    back = to_all(text_part.reshape(plane, pairs, wide + LANES), PLANE)
    came = exchange(send, C, 1)
    pooled_grad, last, totals = local(
        text_gradient, [VMEM, VMEM, VMEM, VMEM],
        ((pairs, width), F32), ((1, width), F32), ((pairs, 2 * LANES), F32),
    )(back, unit_text, text_norm, gain)
    other = exchange(totals, C, 1)
    (blocks,) = local(pack, [SMEM] + [VMEM] * 4, ((depth, pairs, width + 4 * LANES), BF16))(
        lax.axis_index(Z)[None], keep, came, totals, other
    )
    line_back = to_all(blocks, Z)
    behind = from_beside(last, 1)
    (token_grad,) = local(token_rows, [VMEM] * 3, ((tokens, width), F32))(ids, pooled_grad, behind)
    image_grad, gain_grad, scalars = local(
        functools.partial(finish, count=float(total_pairs * total_pairs)), [VMEM] * 3,
        ((pairs, width), F32), ((width,), F32), ((3,), F32),
    )(line_back, unit_image, image_norm)
    return (image_grad, token_grad, gain_grad, scalars)


def solution(mesh):
    finer = Mesh(mesh.devices.reshape(4, 4, 8, 2), DP)
    placed = (P(DP, None), P(DP, None), P(DP), P(DP), P(), P(), P())
    return jax.shard_map(
        per_device,
        mesh=finer,
        in_specs=placed,
        out_specs=(P(DP, None), P(DP, None), P(), P()),
        check_vma=False,
    )
```

```python
import functools

import jax
import jax.numpy as jnp
from jax import lax
from jax.experimental import pallas as pl
from jax.experimental.pallas import tpu as pltpu
from jax.sharding import Mesh
from jax.sharding import PartitionSpec as P

Y, X, Z, C = ("dp_0", "dp_1", "dp_2", "dp_3")
DP = (Y, X, Z, C)
PLANE = (Y, X)
LANES = 128
F32, BF16 = jnp.float32, jnp.bfloat16
VMEM = pl.BlockSpec(memory_space=pltpu.VMEM)
SMEM = pl.BlockSpec(memory_space=pltpu.SMEM)
HBM = pl.BlockSpec(memory_space=pltpu.HBM)

FROM = (0, 2, 4, 6, 1, 3, 5, 7)


def beside(value):
    count = lax.axis_size(DP)
    across = [(i, min(max(i - 1 + 2 * (i % 2), 0), count - 1)) for i in range(count)]
    chip = lax.ppermute(value, DP, across)
    core = exchange(value, C, 1)
    return chip, core


def exchange(value, axis, bit):
    return lax.ppermute(value, axis, [(i, i ^ bit) for i in range(lax.axis_size(axis))])


def to_all(blocks, axes):
    count = lax.axis_size(axes)
    backward = [list(range(count))[::-1]]
    return lax.all_to_all(blocks, axes, 0, 0, tiled=True, axis_index_groups=backward)


def members(ids, pairs, copies):
    slot = lax.broadcasted_iota(jnp.int32, (2 * pairs * copies, 1), 0) % (2 * pairs)
    last = ids[:, ids.shape[1] - 1 :]
    wanted = jnp.where(slot < pairs, slot - (pairs - 1), jnp.where(slot == pairs, -pairs, 1))
    return (ids - last == wanted).astype(F32).astype(BF16)


def id_tile(groups_ref, pairs, for_text):
    row = lax.broadcasted_iota(jnp.int32, (pairs, LANES), 0)
    lane = lax.broadcasted_iota(jnp.int32, (pairs, LANES), 1)
    ids = jnp.zeros((pairs, LANES), jnp.int32)
    for r in range(pairs):
        ids = jnp.where(row == r, groups_ref[r], ids)
    high, low = (ids >> 8) << 8, ids & 255
    if for_text:
        cells = jnp.where(lane < 2, 1, jnp.where(lane == 2, -high, jnp.where(lane == 3, -low, 0)))
    else:
        cells = jnp.where(lane == 0, high, jnp.where(lane == 1, low, jnp.where(lane < 4, 1, 0)))
    return cells.astype(F32).astype(BF16)


def prepare(
    groups_hbm, ids_hbm, image_hbm, tokens_hbm, gain_hbm,
    row_ref, unit_ref, norm_ref, pooled_ref, spill_ref, tile_ref, gain_out, sides_out,
    groups_ref, ids_ref, image_ref, tokens_ref, gain_ref, sems, *, captions,
):
    pairs, width = image_hbm.shape
    moves = [
        pltpu.make_async_copy(source, target, sems.at[i])
        for i, (source, target) in enumerate(
            (
                (image_hbm, image_ref), (groups_hbm, groups_ref), (ids_hbm, ids_ref),
                (tokens_hbm, tokens_ref), (gain_hbm, gain_ref),
            )
        )
    ]
    for move in moves:
        move.start()
    moves[0].wait()
    moves[1].wait()
    image = image_ref[...].astype(F32)
    norm = jnp.sqrt(jnp.sum(image * image, axis=1, keepdims=True))
    unit = image / norm
    unit_ref[...] = unit
    norm_ref[...] = norm
    row_ref[:, :width] = unit.astype(BF16)
    row_ref[:, width:] = id_tile(groups_ref, pairs, False)
    tile_ref[...] = id_tile(groups_ref, pairs, True)
    moves[4].wait()
    gain_out[...] = gain_ref[...][None, :]
    moves[2].wait()
    moves[3].wait()
    last = ids_ref[:, ids_ref.shape[1] - 1 :]
    lane = lax.broadcasted_iota(jnp.int32, (1, LANES), 1)
    odd = (last // pairs) % 2
    sides_out[...] = jnp.where(lane == 0, 1 - odd, jnp.where(last == captions - 1, 0, odd))
    sums = jnp.dot(members(ids_ref[...], pairs, 1), tokens_ref[...], preferred_element_type=F32)
    pooled_ref[...] = sums[:pairs]
    spill_ref[...] = sums[pairs : pairs + 1]


def text_rows(tile_ref, sides_ref, pooled_ref, chip_ref, core_ref, gain_ref, rows_ref, unit_ref, norm_ref):
    pairs, width = pooled_ref.shape
    last = lax.broadcasted_iota(jnp.int32, (pairs, 1), 0) == pairs - 1
    sides = sides_ref[...]
    arrived = jnp.where(sides[:, :1] > 0, core_ref[...], jnp.where(sides[:, 1:2] > 0, chip_ref[...], 0.0))
    pooled = pooled_ref[...] + jnp.where(last, arrived, 0.0)
    embedded = pooled * gain_ref[...]
    norm = jnp.sqrt(jnp.sum(embedded * embedded, axis=1, keepdims=True))
    unit = embedded / norm
    unit_ref[...] = unit
    norm_ref[...] = norm
    low, ids = unit.astype(BF16), tile_ref[...]
    for k in range(rows_ref.shape[0]):
        rows_ref[k, :, :width] = low
        rows_ref[k, :, width:] = ids


def pair_math(knobs_ref, near_ref, far_ref, text_ref, gain_ref, text_out, keep_out, send_out):
    width = gain_ref.shape[1]
    scale = jnp.exp(knobs_ref[:, :1])
    rows = jnp.concatenate([near_ref[...], far_ref[...]], axis=0)
    image, text = rows[:, :width], text_ref[:, :width]
    contract = (((1,), (1,)), ((), ()))
    scaled = scale * lax.dot_general(image, text, contract, preferred_element_type=F32)
    apart = lax.dot_general(
        rows[:, width:], text_ref[:, width:], contract, preferred_element_type=F32
    )
    match = apart == 0.0
    logits = scaled + knobs_ref[:, 1:2]
    margin = jnp.where(match, -logits, logits)
    tail = jnp.exp(-jnp.abs(margin))
    losses = jnp.maximum(margin, 0.0) + jnp.log1p(tail)
    sigmoid = jnp.where(margin >= 0.0, 1.0, tail) / (1.0 + tail)
    coeffs = jnp.where(match, -sigmoid, sigmoid)
    image_part = scale * jnp.dot(coeffs.astype(BF16), text, preferred_element_type=F32)
    text_part = scale * jnp.dot(coeffs.T.astype(BF16), image, preferred_element_type=F32)
    half = keep_out.shape[0]
    keep_out[...] = image_part[:half]
    send_out[...] = image_part[half:].astype(BF16)
    text_out[:, :width] = text_part.astype(BF16)

    unit = text.astype(F32)
    along = jnp.sum(unit * text_part, axis=1, keepdims=True)
    gain_terms = jnp.sum((text_part - unit * along) * unit, axis=0, keepdims=True) / gain_ref[...]
    row = lax.broadcasted_iota(jnp.int32, (8, LANES), 0)
    lane = lax.broadcasted_iota(jnp.int32, (8, LANES), 1)
    first = jnp.zeros((8, LANES), F32)
    for r in range(8):
        first = jnp.where(row == r, gain_terms[:, LANES * r : LANES * (r + 1)], first)
    second = jnp.where(row == 0, gain_terms[:, 8 * LANES : 9 * LANES], 0.0)
    for i, terms in enumerate((losses, coeffs * scaled, coeffs)):
        total = jnp.sum(jnp.sum(terms, axis=0, keepdims=True), axis=1, keepdims=True)
        high = total.astype(BF16).astype(F32)
        second = jnp.where((row == 1) & (lane == i), high, second)
        second = jnp.where((row == 2) & (lane == i), total - high, second)
    packed = jnp.concatenate([first, second], axis=1).astype(BF16)
    for k in range(text_out.shape[0] // 8):
        text_out[8 * k : 8 * (k + 1), width:] = packed


def text_gradient(back_ref, unit_ref, norm_ref, gain_ref, grad_out, last_out, totals_out):
    pairs, width = unit_ref.shape
    total = jnp.sum(back_ref[...].astype(F32), axis=0)
    totals_out[...] = total[:, width:]
    grad, unit = total[:, :width], unit_ref[...]
    grad = grad - unit * jnp.sum(unit * grad, axis=1, keepdims=True)
    grad = grad / norm_ref[...] * gain_ref[...]
    grad_out[...] = grad
    last_out[...] = grad[pairs - 1 :]


def pack(place_ref, keep_ref, came_ref, totals_ref, other_ref, out_ref):
    places, pairs, _ = out_ref.shape
    width = keep_ref.shape[1]
    total = totals_ref[...] + other_ref[...]
    high = total.astype(BF16)
    low = (total - high.astype(F32)).astype(BF16)
    for k in range(places):
        rows = slice(pairs * k, pairs * (k + 1))
        block = keep_ref[rows] + came_ref[rows].astype(F32)
        place = places - 1 - (place_ref[0] ^ FROM[k])
        out_ref[place, :, :width] = block.astype(BF16)
        out_ref[place, :, width : width + 2 * LANES] = high
        out_ref[place, :, width + 2 * LANES :] = low


def token_rows(ids_ref, sides_ref, grad_ref, chip_ref, core_ref, token_out):
    pairs, width = grad_ref.shape
    behind = jnp.where(sides_ref[:, :1] > 0, chip_ref[...], core_ref[...])
    table = jnp.concatenate(
        [grad_ref[...], jnp.broadcast_to(behind, (pairs, width))], axis=0
    )
    high = table.astype(BF16)
    low = (table - high.astype(F32)).astype(BF16)
    token_out[...] = lax.dot_general(
        members(ids_ref[...], pairs, 2),
        jnp.concatenate([high, low], axis=0),
        (((0,), (0,)), ((), ())),
        preferred_element_type=F32,
    )


def finish(back_ref, unit_ref, norm_ref, image_out, gain_out, scalars_out, *, count):
    width = unit_ref.shape[1]
    total = jnp.sum(back_ref[...].astype(F32), axis=0)
    first = total[:, width : width + LANES] + total[:, width + 2 * LANES : width + 3 * LANES]
    second = total[:, width + LANES : width + 2 * LANES] + total[:, width + 3 * LANES :]
    gain_out[...] = jnp.concatenate([first[r] for r in range(8)] + [second[0]])
    scalars_out[...] = ((second[1] + second[2]) / count)[:3]
    grad, unit = total[:, :width], unit_ref[...]
    grad = grad - unit * jnp.sum(unit * grad, axis=1, keepdims=True)
    image_out[...] = grad / norm_ref[...]


def local(kernel, specs, *outs, scratch=()):
    return pl.pallas_call(
        kernel,
        in_specs=specs,
        out_specs=[VMEM] * len(outs),
        out_shape=[jax.ShapeDtypeStruct(*o) for o in outs],
        scratch_shapes=scratch,
        compiler_params=pltpu.CompilerParams(vmem_limit_bytes=16 << 20),
    )


def per_device(image_emb, text_tokens, caption_ids, groups, text_gain, log_scale, logit_bias):
    pairs, width = image_emb.shape
    tokens = text_tokens.shape[0]
    total_pairs = pairs * lax.axis_size(DP)
    plane, depth = lax.axis_size(PLANE), lax.axis_size(Z)
    wide = width + LANES
    ids = caption_ids[None, :]
    row, unit_image, image_norm, pooled, spill, tile, gain, sides = local(
        functools.partial(prepare, captions=total_pairs), [HBM] * 5,
        ((pairs, wide), BF16), ((pairs, width), F32), ((pairs, 1), F32), ((pairs, width), F32),
        ((1, width), F32), ((pairs, LANES), BF16), ((1, width), F32), ((1, LANES), jnp.int32),
        scratch=(
            pltpu.SMEM((pairs,), jnp.int32), pltpu.VMEM((1, tokens), jnp.int32),
            pltpu.VMEM((pairs, width), BF16), pltpu.VMEM((tokens, width), BF16), pltpu.VMEM((width,), F32),
            pltpu.SemaphoreType.DMA((5,)),
        ),
    )(
        *(
            pltpu.with_memory_space_constraint(a, pltpu.HBM)
            for a in (groups, ids, image_emb, text_tokens, text_gain)
        )
    )

    arrived = beside(spill)
    near = [row]
    for step in FROM[1:4]:
        near.append(exchange(row, Z, step))
    near = jnp.concatenate(near, axis=0)
    near = jnp.concatenate([near, exchange(near, Z, 1)], axis=0)
    rows, unit_text, text_norm = local(
        text_rows, [VMEM] * 6,
        ((plane, pairs, wide), BF16), ((pairs, width), F32), ((pairs, 1), F32),
    )(tile, sides, pooled, *arrived, gain)
    texts = to_all(rows, PLANE).reshape(plane * pairs, wide)

    far = exchange(near, C, 1)
    far, log_scale, logit_bias = lax.optimization_barrier((far, log_scale, logit_bias))
    lane = lax.broadcasted_iota(jnp.int32, (1, LANES), 1)
    knobs = jnp.where(lane == 0, log_scale[0], logit_bias[0])
    text_part, keep, send = local(
        pair_math, [VMEM] * 5,
        ((plane * pairs, wide + LANES), BF16), ((depth * pairs, width), F32), ((depth * pairs, width), BF16),
    )(knobs, near, far, texts, gain)

    back = to_all(text_part.reshape(plane, pairs, wide + LANES), PLANE)
    came = exchange(send, C, 1)
    pooled_grad, last, totals = local(
        text_gradient, [VMEM, VMEM, VMEM, VMEM],
        ((pairs, width), F32), ((1, width), F32), ((pairs, 2 * LANES), F32),
    )(back, unit_text, text_norm, gain)
    other = exchange(totals, C, 1)
    (blocks,) = local(pack, [SMEM] + [VMEM] * 4, ((depth, pairs, width + 4 * LANES), BF16))(
        lax.axis_index(Z)[None], keep, came, totals, other
    )
    line_back = to_all(blocks, Z)
    behind = beside(last)
    (token_grad,) = local(token_rows, [VMEM] * 5, ((tokens, width), F32))(ids, sides, pooled_grad, *behind)
    image_grad, gain_grad, scalars = local(
        functools.partial(finish, count=float(total_pairs * total_pairs)), [VMEM] * 3,
        ((pairs, width), F32), ((width,), F32), ((3,), F32),
    )(line_back, unit_image, image_norm)
    return (image_grad, token_grad, gain_grad, scalars)


def solution(mesh):
    finer = Mesh(mesh.devices.reshape(4, 4, 8, 2), DP)
    placed = (P(DP, None), P(DP, None), P(DP), P(DP), P(), P(), P())
    return jax.shard_map(
        per_device,
        mesh=finer,
        in_specs=placed,
        out_specs=(P(DP, None), P(DP, None), P(), P()),
        check_vma=False,
    )
```

```python
import functools

import jax
import jax.numpy as jnp
from jax import lax
from jax.experimental import pallas as pl
from jax.experimental.pallas import tpu as pltpu
from jax.sharding import Mesh
from jax.sharding import PartitionSpec as P

Y, X, Z, C = ("dp_0", "dp_1", "dp_2", "dp_3")
DP = (Y, X, Z, C)
PLANE = (Y, X)
LANES = 128
F32, BF16 = jnp.float32, jnp.bfloat16
VMEM = pl.BlockSpec(memory_space=pltpu.VMEM)
SMEM = pl.BlockSpec(memory_space=pltpu.SMEM)
HBM = pl.BlockSpec(memory_space=pltpu.HBM)

FROM = (0, 2, 4, 6, 1, 3, 5, 7)


def beside(value, ahead):
    count = lax.axis_size(DP)
    across = [(i, i - 1 if i % 2 == 0 else i + 1) for i in range(2, count - 3)]
    across += [(0, 2), (1, 0), (count - 3, count - 1), (count - 2, count - 3), (count - 1, count - 2)]
    chip = lax.ppermute(value, DP, across if ahead else [(b, a) for a, b in across])
    core = exchange(value, C, 1)
    return chip, core


def exchange(value, axis, bit):
    return lax.ppermute(value, axis, [(i, i ^ bit) for i in range(lax.axis_size(axis))])


def to_all(blocks, axes):
    count = lax.axis_size(axes)
    backward = [list(range(count))[::-1]]
    return lax.all_to_all(blocks, axes, 0, 0, tiled=True, axis_index_groups=backward)


def members(ids, pairs, copies):
    slot = lax.broadcasted_iota(jnp.int32, (2 * pairs * copies, 1), 0) % (2 * pairs)
    last = ids[:, ids.shape[1] - 1 :]
    wanted = jnp.where(slot < pairs, slot - (pairs - 1), jnp.where(slot == pairs, -pairs, 1))
    return (ids - last == wanted).astype(F32).astype(BF16)


def id_tile(groups_ref, pairs, for_text):
    row = lax.broadcasted_iota(jnp.int32, (pairs, LANES), 0)
    lane = lax.broadcasted_iota(jnp.int32, (pairs, LANES), 1)
    ids = jnp.zeros((pairs, LANES), jnp.int32)
    for r in range(pairs):
        ids = jnp.where(row == r, groups_ref[r], ids)
    high, low = (ids >> 8) << 8, ids & 255
    if for_text:
        cells = jnp.where(lane < 2, 1, jnp.where(lane == 2, -high, jnp.where(lane == 3, -low, 0)))
    else:
        cells = jnp.where(lane == 0, high, jnp.where(lane == 1, low, jnp.where(lane < 4, 1, 0)))
    return cells.astype(F32).astype(BF16)


def prepare(
    groups_hbm, ids_hbm, image_hbm, tokens_hbm, gain_hbm,
    row_ref, unit_ref, norm_ref, pooled_ref, spill_ref, tile_ref, gain_out, sides_out,
    groups_ref, ids_ref, image_ref, tokens_ref, gain_ref, sems, *, captions,
):
    pairs, width = image_hbm.shape
    moves = [
        pltpu.make_async_copy(source, target, sems.at[i])
        for i, (source, target) in enumerate(
            (
                (image_hbm, image_ref), (groups_hbm, groups_ref), (ids_hbm, ids_ref),
                (tokens_hbm, tokens_ref), (gain_hbm, gain_ref),
            )
        )
    ]
    for move in moves:
        move.start()
    moves[0].wait()
    moves[1].wait()
    image = image_ref[...].astype(F32)
    norm = jnp.sqrt(jnp.sum(image * image, axis=1, keepdims=True))
    unit = image / norm
    unit_ref[...] = unit
    norm_ref[...] = norm
    row_ref[:, :width] = unit.astype(BF16)
    row_ref[:, width:] = id_tile(groups_ref, pairs, False)
    tile_ref[...] = id_tile(groups_ref, pairs, True)
    moves[4].wait()
    gain_out[...] = gain_ref[...][None, :]
    moves[2].wait()
    moves[3].wait()
    last = ids_ref[:, ids_ref.shape[1] - 1 :]
    lane = lax.broadcasted_iota(jnp.int32, (1, LANES), 1)
    odd = (last // pairs) % 2
    sides_out[...] = jnp.where(lane == 0, 1 - odd, jnp.where(last == captions - 1, 0, odd))
    sums = jnp.dot(members(ids_ref[...], pairs, 1), tokens_ref[...], preferred_element_type=F32)
    pooled_ref[...] = sums[:pairs]
    spill_ref[...] = sums[pairs : pairs + 1]


def text_rows(tile_ref, sides_ref, pooled_ref, chip_ref, core_ref, gain_ref, rows_ref, unit_ref, norm_ref):
    pairs, width = pooled_ref.shape
    last = lax.broadcasted_iota(jnp.int32, (pairs, 1), 0) == pairs - 1
    sides = sides_ref[...]
    arrived = jnp.where(sides[:, :1] > 0, core_ref[...], jnp.where(sides[:, 1:2] > 0, chip_ref[...], 0.0))
    pooled = pooled_ref[...] + jnp.where(last, arrived, 0.0)
    embedded = pooled * gain_ref[...]
    norm = jnp.sqrt(jnp.sum(embedded * embedded, axis=1, keepdims=True))
    unit = embedded / norm
    unit_ref[...] = unit
    norm_ref[...] = norm
    low, ids = unit.astype(BF16), tile_ref[...]
    for k in range(rows_ref.shape[0]):
        rows_ref[k, :, :width] = low
        rows_ref[k, :, width:] = ids


def pair_math(knobs_ref, near_ref, far_ref, text_ref, gain_ref, text_out, keep_out, send_out):
    width = gain_ref.shape[1]
    scale = jnp.exp(knobs_ref[:, :1])
    rows = jnp.concatenate([near_ref[...], far_ref[...]], axis=0)
    image, text = rows[:, :width], text_ref[:, :width]
    contract = (((1,), (1,)), ((), ()))
    scaled = scale * lax.dot_general(image, text, contract, preferred_element_type=F32)
    apart = lax.dot_general(
        rows[:, width:], text_ref[:, width:], contract, preferred_element_type=F32
    )
    match = apart == 0.0
    logits = scaled + knobs_ref[:, 1:2]
    margin = jnp.where(match, -logits, logits)
    tail = jnp.exp(-jnp.abs(margin))
    losses = jnp.maximum(margin, 0.0) + jnp.log1p(tail)
    sigmoid = jnp.where(margin >= 0.0, 1.0, tail) / (1.0 + tail)
    coeffs = jnp.where(match, -sigmoid, sigmoid)
    image_part = scale * jnp.dot(coeffs.astype(BF16), text, preferred_element_type=F32)
    text_part = scale * jnp.dot(coeffs.T.astype(BF16), image, preferred_element_type=F32)
    half = keep_out.shape[0]
    keep_out[...] = image_part[:half]
    send_out[...] = image_part[half:].astype(BF16)
    text_out[:, :width] = text_part.astype(BF16)

    unit = text.astype(F32)
    along = jnp.sum(unit * text_part, axis=1, keepdims=True)
    gain_terms = jnp.sum((text_part - unit * along) * unit, axis=0, keepdims=True) / gain_ref[...]
    row = lax.broadcasted_iota(jnp.int32, (8, LANES), 0)
    lane = lax.broadcasted_iota(jnp.int32, (8, LANES), 1)
    first = jnp.zeros((8, LANES), F32)
    for r in range(8):
        first = jnp.where(row == r, gain_terms[:, LANES * r : LANES * (r + 1)], first)
    second = jnp.where(row == 0, gain_terms[:, 8 * LANES : 9 * LANES], 0.0)
    for i, terms in enumerate((losses, coeffs * scaled, coeffs)):
        total = jnp.sum(jnp.sum(terms, axis=0, keepdims=True), axis=1, keepdims=True)
        high = total.astype(BF16).astype(F32)
        second = jnp.where((row == 1) & (lane == i), high, second)
        second = jnp.where((row == 2) & (lane == i), total - high, second)
    packed = jnp.concatenate([first, second], axis=1).astype(BF16)
    for k in range(text_out.shape[0] // 8):
        text_out[8 * k : 8 * (k + 1), width:] = packed


def text_gradient(back_ref, unit_ref, norm_ref, gain_ref, grad_out, last_out, totals_out):
    pairs, width = unit_ref.shape
    total = jnp.sum(back_ref[...].astype(F32), axis=0)
    totals_out[...] = total[:, width:]
    grad, unit = total[:, :width], unit_ref[...]
    grad = grad - unit * jnp.sum(unit * grad, axis=1, keepdims=True)
    grad = grad / norm_ref[...] * gain_ref[...]
    grad_out[...] = grad
    last_out[...] = grad[pairs - 1 :]


def pack(place_ref, keep_ref, came_ref, totals_ref, other_ref, out_ref):
    places, pairs, _ = out_ref.shape
    width = keep_ref.shape[1]
    total = totals_ref[...] + other_ref[...]
    second = total[:, LANES:]
    row = lax.broadcasted_iota(jnp.int32, (pairs, LANES), 0)
    rest, cells = second[1:2] + second[2:3], jnp.where(row == 0, second, 0.0)
    for r in (1, 2, 3):
        part = rest.astype(BF16).astype(F32)
        rest, cells = rest - part, jnp.where(row == r, part, cells)
    packed = jnp.concatenate([total[:, :LANES], cells], axis=1).astype(BF16)
    for k in range(places):
        rows = slice(pairs * k, pairs * (k + 1))
        block = keep_ref[rows] + came_ref[rows].astype(F32)
        place = places - 1 - (place_ref[0] ^ FROM[k])
        out_ref[place, :, :width] = block.astype(BF16)
        out_ref[place, :, width:] = packed


def token_rows(ids_ref, sides_ref, grad_ref, chip_ref, core_ref, token_out):
    pairs, width = grad_ref.shape
    behind = jnp.where(sides_ref[:, :1] > 0, chip_ref[...], core_ref[...])
    table = jnp.concatenate(
        [grad_ref[...], jnp.broadcast_to(behind, (pairs, width))], axis=0
    )
    high = table.astype(BF16)
    low = (table - high.astype(F32)).astype(BF16)
    token_out[...] = lax.dot_general(
        members(ids_ref[...], pairs, 2),
        jnp.concatenate([high, low], axis=0),
        (((0,), (0,)), ((), ())),
        preferred_element_type=F32,
    )


def finish(back_ref, unit_ref, norm_ref, image_out, gain_out, scalars_out, *, count):
    width = unit_ref.shape[1]
    total = jnp.sum(back_ref[...].astype(F32), axis=0)
    first, second = total[:, width : width + LANES], total[:, width + LANES :]
    gain_out[...] = jnp.concatenate([first[r] for r in range(8)] + [second[0]])
    scalars_out[...] = ((second[1] + second[2] + second[3]) / count)[:3]
    grad, unit = total[:, :width], unit_ref[...]
    grad = grad - unit * jnp.sum(unit * grad, axis=1, keepdims=True)
    image_out[...] = grad / norm_ref[...]


def local(kernel, specs, *outs, scratch=()):
    return pl.pallas_call(
        kernel,
        in_specs=specs,
        out_specs=[VMEM] * len(outs),
        out_shape=[jax.ShapeDtypeStruct(*o) for o in outs],
        scratch_shapes=scratch,
        compiler_params=pltpu.CompilerParams(vmem_limit_bytes=16 << 20),
    )


def per_device(image_emb, text_tokens, caption_ids, groups, text_gain, log_scale, logit_bias):
    pairs, width = image_emb.shape
    tokens = text_tokens.shape[0]
    total_pairs = pairs * lax.axis_size(DP)
    plane, depth = lax.axis_size(PLANE), lax.axis_size(Z)
    wide = width + LANES
    ids = caption_ids[None, :]
    row, unit_image, image_norm, pooled, spill, tile, gain, sides = local(
        functools.partial(prepare, captions=total_pairs), [HBM] * 5,
        ((pairs, wide), BF16), ((pairs, width), F32), ((pairs, 1), F32), ((pairs, width), F32),
        ((1, width), F32), ((pairs, LANES), BF16), ((1, width), F32), ((1, LANES), jnp.int32),
        scratch=(
            pltpu.SMEM((pairs,), jnp.int32), pltpu.VMEM((1, tokens), jnp.int32),
            pltpu.VMEM((pairs, width), BF16), pltpu.VMEM((tokens, width), BF16), pltpu.VMEM((width,), F32),
            pltpu.SemaphoreType.DMA((5,)),
        ),
    )(
        *(
            pltpu.with_memory_space_constraint(a, pltpu.HBM)
            for a in (groups, ids, image_emb, text_tokens, text_gain)
        )
    )

    arrived = beside(spill, True)
    near = [row]
    for step in FROM[1:4]:
        near.append(exchange(row, Z, step))
    near = jnp.concatenate(near, axis=0)
    near = jnp.concatenate([near, exchange(near, Z, 1)], axis=0)
    rows, unit_text, text_norm = local(
        text_rows, [VMEM] * 6,
        ((plane, pairs, wide), BF16), ((pairs, width), F32), ((pairs, 1), F32),
    )(tile, sides, pooled, *arrived, gain)
    texts = to_all(rows, PLANE).reshape(plane * pairs, wide)

    far = exchange(near, C, 1)
    far, log_scale, logit_bias = lax.optimization_barrier((far, log_scale, logit_bias))
    lane = lax.broadcasted_iota(jnp.int32, (1, LANES), 1)
    knobs = jnp.where(lane == 0, log_scale[0], logit_bias[0])
    text_part, keep, send = local(
        pair_math, [VMEM] * 5,
        ((plane * pairs, wide + LANES), BF16), ((depth * pairs, width), F32), ((depth * pairs, width), BF16),
    )(knobs, near, far, texts, gain)

    back = to_all(text_part.reshape(plane, pairs, wide + LANES), PLANE)
    came = exchange(send, C, 1)
    pooled_grad, last, totals = local(
        text_gradient, [VMEM, VMEM, VMEM, VMEM],
        ((pairs, width), F32), ((1, width), F32), ((pairs, 2 * LANES), F32),
    )(back, unit_text, text_norm, gain)
    other = exchange(totals, C, 1)
    (blocks,) = local(pack, [SMEM] + [VMEM] * 4, ((depth, pairs, width + 2 * LANES), BF16))(
        lax.axis_index(Z)[None], keep, came, totals, other
    )
    line_back = to_all(blocks, Z)
    behind = beside(last, False)
    (token_grad,) = local(token_rows, [VMEM] * 5, ((tokens, width), F32))(ids, sides, pooled_grad, *behind)
    image_grad, gain_grad, scalars = local(
        functools.partial(finish, count=float(total_pairs * total_pairs)), [VMEM] * 3,
        ((pairs, width), F32), ((width,), F32), ((3,), F32),
    )(line_back, unit_image, image_norm)
    return (image_grad, token_grad, gain_grad, scalars)


def solution(mesh):
    finer = Mesh(mesh.devices.reshape(4, 4, 8, 2), DP)
    placed = (P(DP, None), P(DP, None), P(DP), P(DP), P(), P(), P())
    return jax.shard_map(
        per_device,
        mesh=finer,
        in_specs=placed,
        out_specs=(P(DP, None), P(DP, None), P(), P()),
        check_vma=False,
    )
```

```python
import functools

import jax
import jax.numpy as jnp
from jax import lax
from jax.experimental import pallas as pl
from jax.experimental.pallas import tpu as pltpu
from jax.sharding import Mesh
from jax.sharding import PartitionSpec as P

Y, X, Z, C = ("dp_0", "dp_1", "dp_2", "dp_3")
DP = (Y, X, Z, C)
PLANE = (Y, X)
LANES = 128
F32, BF16 = jnp.float32, jnp.bfloat16
VMEM = pl.BlockSpec(memory_space=pltpu.VMEM)
SMEM = pl.BlockSpec(memory_space=pltpu.SMEM)
HBM = pl.BlockSpec(memory_space=pltpu.HBM)

FROM = (0, 2, 4, 6, 1, 3, 5, 7)


def beside(value, ahead):
    count = lax.axis_size(DP)
    across = [(i, i - 1 if i % 2 == 0 else i + 1) for i in range(2, count - 3)]
    across += [(0, 2), (1, 0), (count - 3, count - 1), (count - 2, count - 3), (count - 1, count - 2)]
    return lax.ppermute(value, DP, across if ahead else [(b, a) for a, b in across])


def exchange(value, axis, bit):
    return lax.ppermute(value, axis, [(i, i ^ bit) for i in range(lax.axis_size(axis))])


def to_all(blocks, axes):
    count = lax.axis_size(axes)
    backward = [list(range(count))[::-1]]
    return lax.all_to_all(blocks, axes, 0, 0, tiled=True, axis_index_groups=backward)


def members(ids, pairs, copies):
    slot = lax.broadcasted_iota(jnp.int32, (2 * pairs * copies, 1), 0) % (2 * pairs)
    last = ids[:, ids.shape[1] - 1 :]
    wanted = jnp.where(slot < pairs, slot - (pairs - 1), jnp.where(slot == pairs, -pairs, 1))
    return (ids - last == wanted).astype(F32).astype(BF16)


def id_tile(groups_ref, pairs, for_text):
    row = lax.broadcasted_iota(jnp.int32, (pairs, LANES), 0)
    lane = lax.broadcasted_iota(jnp.int32, (pairs, LANES), 1)
    ids = jnp.zeros((pairs, LANES), jnp.int32)
    for r in range(pairs):
        ids = jnp.where(row == r, groups_ref[r], ids)
    high, low = (ids >> 8) << 8, ids & 255
    if for_text:
        cells = jnp.where(lane < 2, 1, jnp.where(lane == 2, -high, jnp.where(lane == 3, -low, 0)))
    else:
        cells = jnp.where(lane == 0, high, jnp.where(lane == 1, low, jnp.where(lane < 4, 1, 0)))
    return cells.astype(F32).astype(BF16)


def prepare(
    groups_hbm, ids_hbm, image_hbm, tokens_hbm, gain_hbm,
    row_ref, unit_ref, norm_ref, pooled_ref, spill_ref, tile_ref, gain_out, sides_out,
    groups_ref, ids_ref, image_ref, tokens_ref, gain_ref, sems, *, captions,
):
    pairs, width = image_hbm.shape
    moves = [
        pltpu.make_async_copy(source, target, sems.at[i])
        for i, (source, target) in enumerate(
            (
                (image_hbm, image_ref), (groups_hbm, groups_ref), (ids_hbm, ids_ref),
                (tokens_hbm, tokens_ref), (gain_hbm, gain_ref),
            )
        )
    ]
    for move in moves:
        move.start()
    moves[0].wait()
    moves[1].wait()
    image = image_ref[...].astype(F32)
    norm = jnp.sqrt(jnp.sum(image * image, axis=1, keepdims=True))
    unit = image / norm
    unit_ref[...] = unit
    norm_ref[...] = norm
    row_ref[:pairs, :width] = unit.astype(BF16)
    row_ref[:pairs, width:] = id_tile(groups_ref, pairs, False)
    tile_ref[...] = id_tile(groups_ref, pairs, True)
    moves[4].wait()
    gain_out[...] = gain_ref[...][None, :]
    moves[2].wait()
    moves[3].wait()
    last = ids_ref[:, ids_ref.shape[1] - 1 :]
    lane = lax.broadcasted_iota(jnp.int32, (1, LANES), 1)
    odd = (last // pairs) % 2
    sides_out[...] = jnp.where(lane == 0, 1 - odd, jnp.where(last == captions - 1, 0, odd))
    sums = jnp.dot(members(ids_ref[...], pairs, 1), tokens_ref[...], preferred_element_type=F32)
    pooled_ref[...] = sums[:pairs]
    spill = sums[pairs : pairs + 1]
    spill_ref[...] = spill
    high = spill.astype(BF16).astype(F32)
    row = lax.broadcasted_iota(jnp.int32, (pairs, width), 0)
    cells = jnp.where(row == 0, high, jnp.where(row == 1, spill - high, 0.0))
    row_ref[pairs:, :width] = cells.astype(BF16)
    row_ref[pairs:, width:] = jnp.zeros((pairs, LANES), BF16)


def text_rows(tile_ref, sides_ref, pooled_ref, chip_ref, other_ref, gain_ref, rows_ref, unit_ref, norm_ref):
    pairs, width = pooled_ref.shape
    last = lax.broadcasted_iota(jnp.int32, (pairs, 1), 0) == pairs - 1
    sides = sides_ref[...]
    parts = other_ref[pairs:, :width].astype(F32)
    core = parts[:1] + parts[1:2]
    arrived = jnp.where(sides[:, :1] > 0, core, jnp.where(sides[:, 1:2] > 0, chip_ref[...], 0.0))
    pooled = pooled_ref[...] + jnp.where(last, arrived, 0.0)
    embedded = pooled * gain_ref[...]
    norm = jnp.sqrt(jnp.sum(embedded * embedded, axis=1, keepdims=True))
    unit = embedded / norm
    unit_ref[...] = unit
    norm_ref[...] = norm
    low, ids = unit.astype(BF16), tile_ref[...]
    for k in range(rows_ref.shape[0]):
        rows_ref[k, :, :width] = low
        rows_ref[k, :, width:] = ids


def pair_math(
    knobs_ref, near_ref, far_ref, text_ref, gain_ref, text_hbm, keep_out, send_out, part_ref, packed_ref, sems
):
    width = gain_ref.shape[1]
    scale = jnp.exp(knobs_ref[:, :1])
    rows = jnp.concatenate([near_ref[...], far_ref[...]], axis=0)
    image, text = rows[:, :width], text_ref[:, :width]
    contract = (((1,), (1,)), ((), ()))
    scaled = scale * lax.dot_general(image, text, contract, preferred_element_type=F32)
    apart = lax.dot_general(
        rows[:, width:], text_ref[:, width:], contract, preferred_element_type=F32
    )
    match = apart == 0.0
    logits = scaled + knobs_ref[:, 1:2]
    margin = jnp.where(match, -logits, logits)
    tail = jnp.exp(-jnp.abs(margin))
    losses = jnp.maximum(margin, 0.0) + jnp.log1p(tail)
    sigmoid = jnp.where(margin >= 0.0, 1.0, tail) / (1.0 + tail)
    coeffs = jnp.where(match, -sigmoid, sigmoid)
    text_part = scale * jnp.dot(coeffs.T.astype(BF16), image, preferred_element_type=F32)
    part_ref[...] = text_part.astype(BF16)
    move = pltpu.make_async_copy(part_ref, text_hbm.at[:, pl.ds(0, width)], sems.at[0])
    move.start()

    unit = text.astype(F32)
    along = jnp.sum(unit * text_part, axis=1, keepdims=True)
    gain_terms = jnp.sum((text_part - unit * along) * unit, axis=0, keepdims=True) / gain_ref[...]
    row = lax.broadcasted_iota(jnp.int32, (8, LANES), 0)
    lane = lax.broadcasted_iota(jnp.int32, (8, LANES), 1)
    first = jnp.zeros((8, LANES), F32)
    for r in range(8):
        first = jnp.where(row == r, gain_terms[:, LANES * r : LANES * (r + 1)], first)
    second = jnp.where(row == 0, gain_terms[:, 8 * LANES : 9 * LANES], 0.0)
    for i, terms in enumerate((losses, coeffs * scaled, coeffs)):
        total = jnp.sum(jnp.sum(terms, axis=0, keepdims=True), axis=1, keepdims=True)
        high = total.astype(BF16).astype(F32)
        second = jnp.where((row == 1) & (lane == i), high, second)
        second = jnp.where((row == 2) & (lane == i), total - high, second)
    packed = jnp.concatenate([first, second], axis=1).astype(BF16)
    for k in range(packed_ref.shape[0] // 8):
        packed_ref[8 * k : 8 * (k + 1)] = packed
    rest = pltpu.make_async_copy(packed_ref, text_hbm.at[:, pl.ds(width, 2 * LANES)], sems.at[1])
    rest.start()
    image_part = scale * jnp.dot(coeffs.astype(BF16), text, preferred_element_type=F32)
    for k in range(keep_out.shape[0] // 8):
        keep_out[8 * k : 8 * (k + 1)] = image_part[16 * k : 16 * k + 8]
        send_out[8 * k : 8 * (k + 1)] = image_part[16 * k + 8 : 16 * (k + 1)].astype(BF16)
    move.wait()
    rest.wait()


def text_gradient(back_ref, unit_ref, norm_ref, gain_ref, grad_out, last_out, totals_out):
    pairs, width = unit_ref.shape
    total = jnp.sum(back_ref[...].astype(F32), axis=0)
    totals_out[...] = total[:, width:]
    grad, unit = total[:, :width], unit_ref[...]
    grad = grad - unit * jnp.sum(unit * grad, axis=1, keepdims=True)
    grad = grad / norm_ref[...] * gain_ref[...]
    grad_out[...] = grad
    last_out[...] = grad[pairs - 1 :]


def pack(place_ref, keep_ref, came_ref, totals_ref, other_ref, out_ref):
    places, pairs, _ = out_ref.shape
    width = keep_ref.shape[1]
    total = totals_ref[...] + other_ref[...]
    second = total[:, LANES:]
    row = lax.broadcasted_iota(jnp.int32, (pairs, LANES), 0)
    rest, cells = second[1:2] + second[2:3], jnp.where(row == 0, second, 0.0)
    for r in (1, 2, 3):
        part = rest.astype(BF16).astype(F32)
        rest, cells = rest - part, jnp.where(row == r, part, cells)
    packed = jnp.concatenate([total[:, :LANES], cells], axis=1).astype(BF16)
    for k in range(places):
        rows = slice(pairs * k, pairs * (k + 1))
        block = keep_ref[rows] + came_ref[rows].astype(F32)
        place = places - 1 - (place_ref[0] ^ FROM[k])
        out_ref[place, :, :width] = block.astype(BF16)
        out_ref[place, :, width:] = packed


def token_rows(ids_ref, sides_ref, grad_ref, chip_ref, core_ref, token_out):
    pairs, width = grad_ref.shape
    behind = jnp.where(sides_ref[:, :1] > 0, chip_ref[...], core_ref[...])
    table = jnp.concatenate(
        [grad_ref[...], jnp.broadcast_to(behind, (pairs, width))], axis=0
    )
    high = table.astype(BF16)
    low = (table - high.astype(F32)).astype(BF16)
    token_out[...] = lax.dot_general(
        members(ids_ref[...], pairs, 2),
        jnp.concatenate([high, low], axis=0),
        (((0,), (0,)), ((), ())),
        preferred_element_type=F32,
    )


def finish(back_ref, unit_ref, norm_ref, image_out, gain_out, scalars_out, *, count):
    width = unit_ref.shape[1]
    total = jnp.sum(back_ref[...].astype(F32), axis=0)
    first, second = total[:, width : width + LANES], total[:, width + LANES :]
    gain_out[...] = jnp.concatenate([first[r] for r in range(8)] + [second[0]])
    scalars_out[...] = ((second[1] + second[2] + second[3]) / count)[:3]
    grad, unit = total[:, :width], unit_ref[...]
    grad = grad - unit * jnp.sum(unit * grad, axis=1, keepdims=True)
    image_out[...] = grad / norm_ref[...]


def local(kernel, specs, *outs, scratch=(), to=None):
    return pl.pallas_call(
        kernel,
        in_specs=specs,
        out_specs=to or [VMEM] * len(outs),
        out_shape=[jax.ShapeDtypeStruct(*o) for o in outs],
        scratch_shapes=scratch,
        compiler_params=pltpu.CompilerParams(vmem_limit_bytes=16 << 20),
    )


def per_device(image_emb, text_tokens, caption_ids, groups, text_gain, log_scale, logit_bias):
    pairs, width = image_emb.shape
    tokens = text_tokens.shape[0]
    total_pairs = pairs * lax.axis_size(DP)
    plane, depth = lax.axis_size(PLANE), lax.axis_size(Z)
    wide = width + LANES
    ids = caption_ids[None, :]
    row, unit_image, image_norm, pooled, spill, tile, gain, sides = local(
        functools.partial(prepare, captions=total_pairs), [HBM] * 5,
        ((2 * pairs, wide), BF16), ((pairs, width), F32), ((pairs, 1), F32), ((pairs, width), F32),
        ((1, width), F32), ((pairs, LANES), BF16), ((1, width), F32), ((1, LANES), jnp.int32),
        scratch=(
            pltpu.SMEM((pairs,), jnp.int32), pltpu.VMEM((1, tokens), jnp.int32),
            pltpu.VMEM((pairs, width), BF16), pltpu.VMEM((tokens, width), BF16), pltpu.VMEM((width,), F32),
            pltpu.SemaphoreType.DMA((5,)),
        ),
    )(
        *(
            pltpu.with_memory_space_constraint(a, pltpu.HBM)
            for a in (groups, ids, image_emb, text_tokens, text_gain)
        )
    )

    other = exchange(row, C, 1)
    arrived = beside(spill, True)
    chip = jnp.concatenate([row[:pairs], other[:pairs]], axis=0)
    near = [chip]
    for step in FROM[1:4]:
        near.append(exchange(chip, Z, step))
    near = jnp.concatenate(near, axis=0)
    far = exchange(near, Z, 1)
    far, log_scale, logit_bias = lax.optimization_barrier((far, log_scale, logit_bias))
    lane = lax.broadcasted_iota(jnp.int32, (1, LANES), 1)
    knobs = jnp.where(lane == 0, log_scale[0], logit_bias[0])

    rows, unit_text, text_norm = local(
        text_rows, [VMEM] * 6,
        ((plane, pairs, wide), BF16), ((pairs, width), F32), ((pairs, 1), F32),
    )(tile, sides, pooled, arrived, other, gain)
    texts = to_all(rows, PLANE).reshape(plane * pairs, wide)

    text_part, keep, send = local(
        pair_math, [VMEM] * 5,
        ((plane * pairs, wide + LANES), BF16), ((depth * pairs, width), F32), ((depth * pairs, width), BF16),
        to=[HBM, VMEM, VMEM],
        scratch=(
            pltpu.VMEM((plane * pairs, width), BF16), pltpu.VMEM((plane * pairs, 2 * LANES), BF16),
            pltpu.SemaphoreType.DMA((2,)),
        ),
    )(knobs, near, far, texts, gain)

    back = to_all(text_part.reshape(plane, pairs, wide + LANES), PLANE)
    came = exchange(send, C, 1)
    pooled_grad, last, totals = local(
        text_gradient, [VMEM, VMEM, VMEM, VMEM],
        ((pairs, width), F32), ((1, width), F32), ((pairs, 2 * LANES), F32),
    )(back, unit_text, text_norm, gain)
    other = exchange(totals, C, 1)
    (blocks,) = local(pack, [SMEM] + [VMEM] * 4, ((depth, pairs, width + 2 * LANES), BF16))(
        lax.axis_index(Z)[None], keep, came, totals, other
    )
    line_back = to_all(blocks, Z)
    behind_chip = beside(last, False)
    behind_core = exchange(last, C, 1)
    (token_grad,) = local(token_rows, [VMEM] * 5, ((tokens, width), F32))(ids, sides, pooled_grad, behind_chip, behind_core)
    image_grad, gain_grad, scalars = local(
        functools.partial(finish, count=float(total_pairs * total_pairs)), [VMEM] * 3,
        ((pairs, width), F32), ((width,), F32), ((3,), F32),
    )(line_back, unit_image, image_norm)
    return (image_grad, token_grad, gain_grad, scalars)


def solution(mesh):
    finer = Mesh(mesh.devices.reshape(4, 4, 8, 2), DP)
    placed = (P(DP, None), P(DP, None), P(DP), P(DP), P(), P(), P())
    return jax.shard_map(
        per_device,
        mesh=finer,
        in_specs=placed,
        out_specs=(P(DP, None), P(DP, None), P(), P()),
        check_vma=False,
    )
```

```python
import functools

import jax
import jax.numpy as jnp
from jax import lax
from jax.experimental import pallas as pl
from jax.experimental.pallas import tpu as pltpu
from jax.sharding import Mesh
from jax.sharding import PartitionSpec as P

Y, X, Z, C = ("dp_0", "dp_1", "dp_2", "dp_3")
DP = (Y, X, Z, C)
PLANE = (Y, X)
LANES = 128
F32, BF16 = jnp.float32, jnp.bfloat16
VMEM = pl.BlockSpec(memory_space=pltpu.VMEM)
SMEM = pl.BlockSpec(memory_space=pltpu.SMEM)
HBM = pl.BlockSpec(memory_space=pltpu.HBM)

FROM = (0, 2, 4, 6, 1, 3, 5, 7)


def beside(value, ahead):
    count = lax.axis_size(DP)
    across = [(i, i - 1 if i % 2 == 0 else i + 1) for i in range(2, count - 3)]
    across += [(0, 2), (1, 0), (count - 3, count - 1), (count - 2, count - 3), (count - 1, count - 2)]
    return lax.ppermute(value, DP, across if ahead else [(b, a) for a, b in across])


def exchange(value, axis, bit):
    return lax.ppermute(value, axis, [(i, i ^ bit) for i in range(lax.axis_size(axis))])


def to_all(blocks, axes):
    count = lax.axis_size(axes)
    backward = [list(range(count))[::-1]]
    return lax.all_to_all(blocks, axes, 0, 0, tiled=True, axis_index_groups=backward)


def members(ids, pairs, copies):
    slot = lax.broadcasted_iota(jnp.int32, (2 * pairs * copies, 1), 0) % (2 * pairs)
    last = ids[:, ids.shape[1] - 1 :]
    wanted = jnp.where(slot < pairs, slot - (pairs - 1), jnp.where(slot == pairs, -pairs, 1))
    return (ids - last == wanted).astype(F32).astype(BF16)


def id_tile(groups_ref, pairs, for_text):
    row = lax.broadcasted_iota(jnp.int32, (pairs, LANES), 0)
    lane = lax.broadcasted_iota(jnp.int32, (pairs, LANES), 1)
    ids = jnp.zeros((pairs, LANES), jnp.int32)
    for r in range(pairs):
        ids = jnp.where(row == r, groups_ref[r], ids)
    high, low = (ids >> 8) << 8, ids & 255
    if for_text:
        cells = jnp.where(lane < 2, 1, jnp.where(lane == 2, -high, jnp.where(lane == 3, -low, 0)))
    else:
        cells = jnp.where(lane == 0, high, jnp.where(lane == 1, low, jnp.where(lane < 4, 1, 0)))
    return cells.astype(F32).astype(BF16)


def prepare(
    groups_hbm, ids_hbm, image_hbm, tokens_hbm, gain_hbm,
    row_ref, unit_ref, norm_ref, pooled_ref, spill_ref, tile_ref, gain_out, sides_out,
    groups_ref, ids_ref, image_ref, tokens_ref, gain_ref, sems, *, captions,
):
    pairs, width = image_hbm.shape
    moves = [
        pltpu.make_async_copy(source, target, sems.at[i])
        for i, (source, target) in enumerate(
            (
                (image_hbm, image_ref), (groups_hbm, groups_ref), (ids_hbm, ids_ref),
                (tokens_hbm, tokens_ref), (gain_hbm, gain_ref),
            )
        )
    ]
    for move in moves:
        move.start()
    moves[0].wait()
    moves[1].wait()
    image = image_ref[...].astype(F32)
    norm = jnp.sqrt(jnp.sum(image * image, axis=1, keepdims=True))
    unit = image / norm
    unit_ref[...] = unit
    norm_ref[...] = norm
    row_ref[:pairs, :width] = unit.astype(BF16)
    row_ref[:pairs, width:] = id_tile(groups_ref, pairs, False)
    tile_ref[...] = id_tile(groups_ref, pairs, True)
    moves[4].wait()
    gain_out[...] = gain_ref[...][None, :]
    moves[2].wait()
    moves[3].wait()
    last = ids_ref[:, ids_ref.shape[1] - 1 :]
    lane = lax.broadcasted_iota(jnp.int32, (1, LANES), 1)
    odd = (last // pairs) % 2
    sides_out[...] = jnp.where(lane == 0, 1 - odd, jnp.where(last == captions - 1, 0, odd))
    sums = jnp.dot(members(ids_ref[...], pairs, 1), tokens_ref[...], preferred_element_type=F32)
    pooled_ref[...] = sums[:pairs]
    spill = sums[pairs : pairs + 1]
    spill_ref[...] = spill
    high = spill.astype(BF16).astype(F32)
    row = lax.broadcasted_iota(jnp.int32, (pairs, width), 0)
    cells = jnp.where(row == 0, high, jnp.where(row == 1, spill - high, 0.0))
    row_ref[pairs:, :width] = cells.astype(BF16)
    row_ref[pairs:, width:] = jnp.zeros((pairs, LANES), BF16)


def text_rows(tile_ref, sides_ref, pooled_ref, chip_ref, other_ref, gain_ref, rows_ref, unit_ref, norm_ref):
    pairs, width = pooled_ref.shape
    last = lax.broadcasted_iota(jnp.int32, (pairs, 1), 0) == pairs - 1
    sides = sides_ref[...]
    parts = other_ref[pairs:, :width].astype(F32)
    core = parts[:1] + parts[1:2]
    arrived = jnp.where(sides[:, :1] > 0, core, jnp.where(sides[:, 1:2] > 0, chip_ref[...], 0.0))
    pooled = pooled_ref[...] + jnp.where(last, arrived, 0.0)
    embedded = pooled * gain_ref[...]
    norm = jnp.sqrt(jnp.sum(embedded * embedded, axis=1, keepdims=True))
    unit = embedded / norm
    unit_ref[...] = unit
    norm_ref[...] = norm
    low, ids = unit.astype(BF16), tile_ref[...]
    for k in range(rows_ref.shape[0]):
        rows_ref[k, :, :width] = low
        rows_ref[k, :, width:] = ids


def pair_math(
    knobs_ref, near_ref, far_ref, text_ref, gain_ref, text_hbm, keep_out, send_out, part_ref, packed_ref, sems
):
    width = gain_ref.shape[1]
    scale = jnp.exp(knobs_ref[:, :1])
    rows = jnp.concatenate([near_ref[...], far_ref[...]], axis=0)
    image, text = rows[:, :width], text_ref[:, :width]
    contract = (((1,), (1,)), ((), ()))
    scaled = scale * lax.dot_general(image, text, contract, preferred_element_type=F32)
    apart = lax.dot_general(
        rows[:, width:], text_ref[:, width:], contract, preferred_element_type=F32
    )
    match = apart == 0.0
    logits = scaled + knobs_ref[:, 1:2]
    margin = jnp.where(match, -logits, logits)
    tail = jnp.exp(-jnp.abs(margin))
    losses = jnp.maximum(margin, 0.0) + jnp.log1p(tail)
    sigmoid = jnp.where(margin >= 0.0, 1.0, tail) / (1.0 + tail)
    coeffs = jnp.where(match, -sigmoid, sigmoid)
    text_part = scale * jnp.dot(coeffs.T.astype(BF16), image, preferred_element_type=F32)
    part_ref[...] = text_part.astype(BF16)
    move = pltpu.make_async_copy(part_ref, text_hbm.at[:, pl.ds(0, width)], sems.at[0])
    move.start()

    unit = text.astype(F32)
    along = jnp.sum(unit * text_part, axis=1, keepdims=True)
    gain_terms = jnp.sum((text_part - unit * along) * unit, axis=0, keepdims=True) / gain_ref[...]
    row = lax.broadcasted_iota(jnp.int32, (8, LANES), 0)
    lane = lax.broadcasted_iota(jnp.int32, (8, LANES), 1)
    first = jnp.zeros((8, LANES), F32)
    for r in range(8):
        first = jnp.where(row == r, gain_terms[:, LANES * r : LANES * (r + 1)], first)
    second = jnp.where(row == 0, gain_terms[:, 8 * LANES : 9 * LANES], 0.0)
    for i, terms in enumerate((losses, coeffs * scaled, coeffs)):
        total = jnp.sum(jnp.sum(terms, axis=0, keepdims=True), axis=1, keepdims=True)
        high = total.astype(BF16).astype(F32)
        second = jnp.where((row == 1) & (lane == i), high, second)
        second = jnp.where((row == 2) & (lane == i), total - high, second)
    packed = jnp.concatenate([first, second], axis=1).astype(BF16)
    for k in range(packed_ref.shape[0] // 8):
        packed_ref[8 * k : 8 * (k + 1)] = packed
    rest = pltpu.make_async_copy(packed_ref, text_hbm.at[:, pl.ds(width, 2 * LANES)], sems.at[1])
    rest.start()
    image_part = scale * jnp.dot(coeffs.astype(BF16), text, preferred_element_type=F32)
    for k in range(keep_out.shape[0] // 8):
        own = 16 * k + (8 if k % 4 == 3 else 0)
        far = 32 * k + 8 - own
        keep_out[8 * k : 8 * (k + 1)] = image_part[own : own + 8]
        send_out[8 * k : 8 * (k + 1)] = image_part[far : far + 8].astype(BF16)
    move.wait()
    rest.wait()


def text_gradient(back_ref, unit_ref, norm_ref, gain_ref, grad_out, last_out, totals_out):
    pairs, width = unit_ref.shape
    total = jnp.sum(back_ref[...].astype(F32), axis=0)
    totals_out[...] = total[:, width:]
    grad, unit = total[:, :width], unit_ref[...]
    grad = grad - unit * jnp.sum(unit * grad, axis=1, keepdims=True)
    grad = grad / norm_ref[...] * gain_ref[...]
    grad_out[...] = grad
    last_out[...] = grad[pairs - 1 :]


def pack(place_ref, keep_ref, came_ref, totals_ref, other_ref, out_ref):
    places, pairs, _ = out_ref.shape
    width = keep_ref.shape[1]
    total = totals_ref[...] + other_ref[...]
    second = total[:, LANES:]
    row = lax.broadcasted_iota(jnp.int32, (pairs, LANES), 0)
    rest, cells = second[1:2] + second[2:3], jnp.where(row == 0, second, 0.0)
    for r in (1, 2, 3):
        part = rest.astype(BF16).astype(F32)
        rest, cells = rest - part, jnp.where(row == r, part, cells)
    packed = jnp.concatenate([total[:, :LANES], cells], axis=1).astype(BF16)
    for k in range(places):
        there = k ^ 2 if k % 2 else k
        block = keep_ref[pairs * k : pairs * (k + 1)]
        block = block + came_ref[pairs * there : pairs * (there + 1)].astype(F32)
        turn = (1 - place_ref[0] % 2) * 4 if k % 2 else 0
        place = places - 1 - ((place_ref[0] // 2) ^ FROM[k] ^ turn)
        out_ref[place, :, :width] = block.astype(BF16)
        out_ref[place, :, width:] = packed


def token_rows(ids_ref, sides_ref, grad_ref, chip_ref, core_ref, token_out):
    pairs, width = grad_ref.shape
    behind = jnp.where(sides_ref[:, :1] > 0, chip_ref[...], core_ref[...])
    table = jnp.concatenate(
        [grad_ref[...], jnp.broadcast_to(behind, (pairs, width))], axis=0
    )
    high = table.astype(BF16)
    low = (table - high.astype(F32)).astype(BF16)
    token_out[...] = lax.dot_general(
        members(ids_ref[...], pairs, 2),
        jnp.concatenate([high, low], axis=0),
        (((0,), (0,)), ((), ())),
        preferred_element_type=F32,
    )


def finish(back_ref, unit_ref, norm_ref, image_out, gain_out, scalars_out, *, count):
    width = unit_ref.shape[1]
    total = jnp.sum(back_ref[...].astype(F32), axis=0)
    first, second = total[:, width : width + LANES], total[:, width + LANES :]
    gain_out[...] = jnp.concatenate([first[r] for r in range(8)] + [second[0]])
    scalars_out[...] = ((second[1] + second[2] + second[3]) / count)[:3]
    grad, unit = total[:, :width], unit_ref[...]
    grad = grad - unit * jnp.sum(unit * grad, axis=1, keepdims=True)
    image_out[...] = grad / norm_ref[...]


def local(kernel, specs, *outs, scratch=(), to=None):
    return pl.pallas_call(
        kernel,
        in_specs=specs,
        out_specs=to or [VMEM] * len(outs),
        out_shape=[jax.ShapeDtypeStruct(*o) for o in outs],
        scratch_shapes=scratch,
        compiler_params=pltpu.CompilerParams(vmem_limit_bytes=16 << 20),
    )


def per_device(image_emb, text_tokens, caption_ids, groups, text_gain, log_scale, logit_bias):
    pairs, width = image_emb.shape
    tokens = text_tokens.shape[0]
    total_pairs = pairs * lax.axis_size(DP)
    plane, depth = lax.axis_size(PLANE), lax.axis_size(Z)
    wide = width + LANES
    ids = caption_ids[None, :]
    row, unit_image, image_norm, pooled, spill, tile, gain, sides = local(
        functools.partial(prepare, captions=total_pairs), [HBM] * 5,
        ((2 * pairs, wide), BF16), ((pairs, width), F32), ((pairs, 1), F32), ((pairs, width), F32),
        ((1, width), F32), ((pairs, LANES), BF16), ((1, width), F32), ((1, LANES), jnp.int32),
        scratch=(
            pltpu.SMEM((pairs,), jnp.int32), pltpu.VMEM((1, tokens), jnp.int32),
            pltpu.VMEM((pairs, width), BF16), pltpu.VMEM((tokens, width), BF16), pltpu.VMEM((width,), F32),
            pltpu.SemaphoreType.DMA((5,)),
        ),
    )(
        *(
            pltpu.with_memory_space_constraint(a, pltpu.HBM)
            for a in (groups, ids, image_emb, text_tokens, text_gain)
        )
    )

    other = exchange(row, C, 1)
    arrived = beside(spill, True)
    chip = jnp.concatenate([row[:pairs], other[:pairs]], axis=0)
    line = lax.axis_size((Z, C))
    first = lax.ppermute(chip, (Z, C), [(i, i ^ (4 if i % 2 else 12)) for i in range(line)])
    second = exchange(chip, Z, 4)
    third = exchange(first, C, 1)
    near = jnp.concatenate([chip, first, second, third], axis=0)
    far = exchange(near, Z, 1)
    far, log_scale, logit_bias = lax.optimization_barrier((far, log_scale, logit_bias))
    lane = lax.broadcasted_iota(jnp.int32, (1, LANES), 1)
    knobs = jnp.where(lane == 0, log_scale[0], logit_bias[0])

    rows, unit_text, text_norm = local(
        text_rows, [VMEM] * 6,
        ((plane, pairs, wide), BF16), ((pairs, width), F32), ((pairs, 1), F32),
    )(tile, sides, pooled, arrived, other, gain)
    texts = to_all(rows, PLANE).reshape(plane * pairs, wide)

    text_part, keep, send = local(
        pair_math, [VMEM] * 5,
        ((plane * pairs, wide + LANES), BF16), ((depth * pairs, width), F32), ((depth * pairs, width), BF16),
        to=[HBM, VMEM, VMEM],
        scratch=(
            pltpu.VMEM((plane * pairs, width), BF16), pltpu.VMEM((plane * pairs, 2 * LANES), BF16),
            pltpu.SemaphoreType.DMA((2,)),
        ),
    )(knobs, near, far, texts, gain)

    back = to_all(text_part.reshape(plane, pairs, wide + LANES), PLANE)
    came = exchange(send, C, 1)
    pooled_grad, last, totals = local(
        text_gradient, [VMEM, VMEM, VMEM, VMEM],
        ((pairs, width), F32), ((1, width), F32), ((pairs, 2 * LANES), F32),
    )(back, unit_text, text_norm, gain)
    other = exchange(totals, C, 1)
    (blocks,) = local(pack, [SMEM] + [VMEM] * 4, ((depth, pairs, width + 2 * LANES), BF16))(
        lax.axis_index((Z, C))[None], keep, came, totals, other
    )
    line_back = to_all(blocks, Z)
    behind_chip = beside(last, False)
    behind_core = exchange(last, C, 1)
    (token_grad,) = local(token_rows, [VMEM] * 5, ((tokens, width), F32))(ids, sides, pooled_grad, behind_chip, behind_core)
    image_grad, gain_grad, scalars = local(
        functools.partial(finish, count=float(total_pairs * total_pairs)), [VMEM] * 3,
        ((pairs, width), F32), ((width,), F32), ((3,), F32),
    )(line_back, unit_image, image_norm)
    return (image_grad, token_grad, gain_grad, scalars)


def solution(mesh):
    finer = Mesh(mesh.devices.reshape(4, 4, 8, 2), DP)
    placed = (P(DP, None), P(DP, None), P(DP), P(DP), P(), P(), P())
    return jax.shard_map(
        per_device,
        mesh=finer,
        in_specs=placed,
        out_specs=(P(DP, None), P(DP, None), P(), P()),
        check_vma=False,
    )
```

```python
import functools

import jax
import jax.numpy as jnp
from jax import lax
from jax.experimental import pallas as pl
from jax.experimental.pallas import tpu as pltpu
from jax.sharding import Mesh
from jax.sharding import PartitionSpec as P

Y, X, Z, C = ("dp_0", "dp_1", "dp_2", "dp_3")
DP = (Y, X, Z, C)
PLANE = (Y, X)
LANES = 128
F32, BF16 = jnp.float32, jnp.bfloat16
VMEM = pl.BlockSpec(memory_space=pltpu.VMEM)
SMEM = pl.BlockSpec(memory_space=pltpu.SMEM)
HBM = pl.BlockSpec(memory_space=pltpu.HBM)

FROM = (0, 2, 4, 6, 1, 3, 5, 7)


def beside(value, ahead):
    count = lax.axis_size(DP)
    across = [(i, i - 1 if i % 2 == 0 else i + 1) for i in range(2, count - 3)]
    across += [(0, 2), (1, 0), (count - 3, count - 1), (count - 2, count - 3), (count - 1, count - 2)]
    return lax.ppermute(value, DP, across if ahead else [(b, a) for a, b in across])


def exchange(value, axis, bit):
    return lax.ppermute(value, axis, [(i, i ^ bit) for i in range(lax.axis_size(axis))])


def to_all(blocks, axes):
    count = lax.axis_size(axes)
    backward = [list(range(count))[::-1]]
    return lax.all_to_all(blocks, axes, 0, 0, tiled=True, axis_index_groups=backward)


def members(ids, pairs, copies):
    slot = lax.broadcasted_iota(jnp.int32, (2 * pairs * copies, 1), 0) % (2 * pairs)
    last = ids[:, ids.shape[1] - 1 :]
    wanted = jnp.where(slot < pairs, slot - (pairs - 1), jnp.where(slot == pairs, -pairs, 1))
    return (ids - last == wanted).astype(F32).astype(BF16)


def id_tile(groups_ref, pairs, for_text):
    row = lax.broadcasted_iota(jnp.int32, (pairs, LANES), 0)
    lane = lax.broadcasted_iota(jnp.int32, (pairs, LANES), 1)
    ids = jnp.zeros((pairs, LANES), jnp.int32)
    for r in range(pairs):
        ids = jnp.where(row == r, groups_ref[r], ids)
    high, low = (ids >> 8) << 8, ids & 255
    if for_text:
        cells = jnp.where(lane < 2, 1, jnp.where(lane == 2, -high, jnp.where(lane == 3, -low, 0)))
    else:
        cells = jnp.where(lane == 0, high, jnp.where(lane == 1, low, jnp.where(lane < 4, 1, 0)))
    return cells.astype(F32).astype(BF16)


def prepare(
    groups_hbm, ids_hbm, image_hbm, tokens_hbm, gain_hbm,
    row_ref, unit_ref, norm_ref, pooled_ref, spill_ref, tile_ref, gain_out, sides_out,
    groups_ref, ids_ref, image_ref, tokens_ref, gain_ref, sems, *, captions,
):
    pairs, width = image_hbm.shape
    moves = [
        pltpu.make_async_copy(source, target, sems.at[i])
        for i, (source, target) in enumerate(
            (
                (image_hbm, image_ref), (groups_hbm, groups_ref), (ids_hbm, ids_ref),
                (tokens_hbm, tokens_ref), (gain_hbm, gain_ref),
            )
        )
    ]
    for move in moves:
        move.start()
    moves[0].wait()
    moves[1].wait()
    image = image_ref[...].astype(F32)
    norm = jnp.sqrt(jnp.sum(image * image, axis=1, keepdims=True))
    unit = image / norm
    unit_ref[...] = unit
    norm_ref[...] = norm
    row_ref[:pairs, :width] = unit.astype(BF16)
    row_ref[:pairs, width:] = id_tile(groups_ref, pairs, False)
    tile_ref[...] = id_tile(groups_ref, pairs, True)
    moves[4].wait()
    gain_out[...] = gain_ref[...][None, :]
    moves[2].wait()
    moves[3].wait()
    last = ids_ref[:, ids_ref.shape[1] - 1 :]
    lane = lax.broadcasted_iota(jnp.int32, (1, LANES), 1)
    odd = (last // pairs) % 2
    sides_out[...] = jnp.where(lane == 0, 1 - odd, jnp.where(last == captions - 1, 0, odd))
    sums = jnp.dot(members(ids_ref[...], pairs, 1), tokens_ref[...], preferred_element_type=F32)
    pooled_ref[...] = sums[:pairs]
    spill = sums[pairs : pairs + 1]
    spill_ref[...] = spill
    high = spill.astype(BF16).astype(F32)
    row = lax.broadcasted_iota(jnp.int32, (pairs, width), 0)
    cells = jnp.where(row == 0, high, jnp.where(row == 1, spill - high, 0.0))
    row_ref[pairs:, :width] = cells.astype(BF16)
    row_ref[pairs:, width:] = jnp.zeros((pairs, LANES), BF16)


def text_rows(tile_ref, sides_ref, pooled_ref, chip_ref, other_ref, gain_ref, rows_ref, unit_ref, norm_ref):
    pairs, width = pooled_ref.shape
    last = lax.broadcasted_iota(jnp.int32, (pairs, 1), 0) == pairs - 1
    sides = sides_ref[...]
    parts = other_ref[pairs:, :width].astype(F32)
    core = parts[:1] + parts[1:2]
    arrived = jnp.where(sides[:, :1] > 0, core, jnp.where(sides[:, 1:2] > 0, chip_ref[...], 0.0))
    pooled = pooled_ref[...] + jnp.where(last, arrived, 0.0)
    embedded = pooled * gain_ref[...]
    norm = jnp.sqrt(jnp.sum(embedded * embedded, axis=1, keepdims=True))
    unit = embedded / norm
    unit_ref[...] = unit
    norm_ref[...] = norm
    low, ids = unit.astype(BF16), tile_ref[...]
    for k in range(rows_ref.shape[0]):
        rows_ref[k, :, :width] = low
        rows_ref[k, :, width:] = ids


def pair_math(
    knobs_ref, chip_ref, even_ref, beside_ref, far_ref, text_ref, gain_ref, text_hbm, keep_out, send_out, part_ref, packed_ref, sems
):
    width = gain_ref.shape[1]
    scale = jnp.exp(knobs_ref[:, :1])
    rows = jnp.concatenate([chip_ref[...], even_ref[...], beside_ref[...], far_ref[...]], axis=0)
    image, text = rows[:, :width], text_ref[:, :width]
    contract = (((1,), (1,)), ((), ()))
    scaled = scale * lax.dot_general(image, text, contract, preferred_element_type=F32)
    apart = lax.dot_general(
        rows[:, width:], text_ref[:, width:], contract, preferred_element_type=F32
    )
    match = apart == 0.0
    logits = scaled + knobs_ref[:, 1:2]
    margin = jnp.where(match, -logits, logits)
    tail = jnp.exp(-jnp.abs(margin))
    losses = jnp.maximum(margin, 0.0) + jnp.log1p(tail)
    sigmoid = jnp.where(margin >= 0.0, 1.0, tail) / (1.0 + tail)
    coeffs = jnp.where(match, -sigmoid, sigmoid)
    text_part = scale * jnp.dot(coeffs.T.astype(BF16), image, preferred_element_type=F32)
    part_ref[...] = text_part.astype(BF16)
    move = pltpu.make_async_copy(part_ref, text_hbm.at[:, pl.ds(0, width)], sems.at[0])
    move.start()

    unit = text.astype(F32)
    along = jnp.sum(unit * text_part, axis=1, keepdims=True)
    gain_terms = jnp.sum((text_part - unit * along) * unit, axis=0, keepdims=True) / gain_ref[...]
    row = lax.broadcasted_iota(jnp.int32, (8, LANES), 0)
    lane = lax.broadcasted_iota(jnp.int32, (8, LANES), 1)
    first = jnp.zeros((8, LANES), F32)
    for r in range(8):
        first = jnp.where(row == r, gain_terms[:, LANES * r : LANES * (r + 1)], first)
    second = jnp.where(row == 0, gain_terms[:, 8 * LANES : 9 * LANES], 0.0)
    for i, terms in enumerate((losses, coeffs * scaled, coeffs)):
        total = jnp.sum(jnp.sum(terms, axis=0, keepdims=True), axis=1, keepdims=True)
        high = total.astype(BF16).astype(F32)
        second = jnp.where((row == 1) & (lane == i), high, second)
        second = jnp.where((row == 2) & (lane == i), total - high, second)
    packed = jnp.concatenate([first, second], axis=1).astype(BF16)
    for k in range(packed_ref.shape[0] // 8):
        packed_ref[8 * k : 8 * (k + 1)] = packed
    rest = pltpu.make_async_copy(packed_ref, text_hbm.at[:, pl.ds(width, 2 * LANES)], sems.at[1])
    rest.start()
    image_part = scale * jnp.dot(coeffs.astype(BF16), text, preferred_element_type=F32)
    for k in range(keep_out.shape[0] // 8):
        keep_out[8 * k : 8 * (k + 1)] = image_part[16 * k : 16 * k + 8]
        send_out[8 * k : 8 * (k + 1)] = image_part[16 * k + 8 : 16 * (k + 1)].astype(BF16)
    move.wait()
    rest.wait()


def text_gradient(back_ref, unit_ref, norm_ref, gain_ref, grad_out, last_out, totals_out):
    pairs, width = unit_ref.shape
    total = jnp.sum(back_ref[...].astype(F32), axis=0)
    totals_out[...] = total[:, width:]
    grad, unit = total[:, :width], unit_ref[...]
    grad = grad - unit * jnp.sum(unit * grad, axis=1, keepdims=True)
    grad = grad / norm_ref[...] * gain_ref[...]
    grad_out[...] = grad
    last_out[...] = grad[pairs - 1 :]


def pack(place_ref, keep_ref, came_ref, totals_ref, other_ref, out_ref):
    places, pairs, _ = out_ref.shape
    width = keep_ref.shape[1]
    total = totals_ref[...] + other_ref[...]
    second = total[:, LANES:]
    row = lax.broadcasted_iota(jnp.int32, (pairs, LANES), 0)
    rest, cells = second[1:2] + second[2:3], jnp.where(row == 0, second, 0.0)
    for r in (1, 2, 3):
        part = rest.astype(BF16).astype(F32)
        rest, cells = rest - part, jnp.where(row == r, part, cells)
    packed = jnp.concatenate([total[:, :LANES], cells], axis=1).astype(BF16)
    for k in range(places):
        moved = k % 4 in (1, 2)
        there = k ^ 3 if moved else k
        block = keep_ref[pairs * k : pairs * (k + 1)]
        block = block + came_ref[pairs * there : pairs * (there + 1)].astype(F32)
        turn = (1 - place_ref[0] % 2) * 6 if moved else 0
        place = places - 1 - ((place_ref[0] // 2) ^ FROM[k] ^ turn)
        out_ref[place, :, :width] = block.astype(BF16)
        out_ref[place, :, width:] = packed


def token_rows(ids_ref, sides_ref, grad_ref, chip_ref, core_ref, token_out):
    pairs, width = grad_ref.shape
    behind = jnp.where(sides_ref[:, :1] > 0, chip_ref[...], core_ref[...])
    table = jnp.concatenate(
        [grad_ref[...], jnp.broadcast_to(behind, (pairs, width))], axis=0
    )
    high = table.astype(BF16)
    low = (table - high.astype(F32)).astype(BF16)
    token_out[...] = lax.dot_general(
        members(ids_ref[...], pairs, 2),
        jnp.concatenate([high, low], axis=0),
        (((0,), (0,)), ((), ())),
        preferred_element_type=F32,
    )


def finish(back_ref, unit_ref, norm_ref, image_out, gain_out, scalars_out, *, count):
    width = unit_ref.shape[1]
    total = jnp.sum(back_ref[...].astype(F32), axis=0)
    first, second = total[:, width : width + LANES], total[:, width + LANES :]
    gain_out[...] = jnp.concatenate([first[r] for r in range(8)] + [second[0]])
    scalars_out[...] = ((second[1] + second[2] + second[3]) / count)[:3]
    grad, unit = total[:, :width], unit_ref[...]
    grad = grad - unit * jnp.sum(unit * grad, axis=1, keepdims=True)
    image_out[...] = grad / norm_ref[...]


def local(kernel, specs, *outs, scratch=(), to=None):
    return pl.pallas_call(
        kernel,
        in_specs=specs,
        out_specs=to or [VMEM] * len(outs),
        out_shape=[jax.ShapeDtypeStruct(*o) for o in outs],
        scratch_shapes=scratch,
        compiler_params=pltpu.CompilerParams(vmem_limit_bytes=16 << 20),
    )


def per_device(image_emb, text_tokens, caption_ids, groups, text_gain, log_scale, logit_bias):
    pairs, width = image_emb.shape
    tokens = text_tokens.shape[0]
    total_pairs = pairs * lax.axis_size(DP)
    plane, depth = lax.axis_size(PLANE), lax.axis_size(Z)
    wide = width + LANES
    ids = caption_ids[None, :]
    row, unit_image, image_norm, pooled, spill, tile, gain, sides = local(
        functools.partial(prepare, captions=total_pairs), [HBM] * 5,
        ((2 * pairs, wide), BF16), ((pairs, width), F32), ((pairs, 1), F32), ((pairs, width), F32),
        ((1, width), F32), ((pairs, LANES), BF16), ((1, width), F32), ((1, LANES), jnp.int32),
        scratch=(
            pltpu.SMEM((pairs,), jnp.int32), pltpu.VMEM((1, tokens), jnp.int32),
            pltpu.VMEM((pairs, width), BF16), pltpu.VMEM((tokens, width), BF16), pltpu.VMEM((width,), F32),
            pltpu.SemaphoreType.DMA((5,)),
        ),
    )(
        *(
            pltpu.with_memory_space_constraint(a, pltpu.HBM)
            for a in (groups, ids, image_emb, text_tokens, text_gain)
        )
    )

    other = exchange(row, C, 1)
    arrived = beside(spill, True)
    chip = jnp.concatenate([row[:pairs], other[:pairs]], axis=0)
    line = lax.axis_size((Z, C))

    def by_core(value, zero, one):
        return lax.ppermute(value, (Z, C), [(i, i ^ 2 * (one if i % 2 else zero)) for i in range(line)])

    def turned(block):
        return jnp.concatenate([block[pairs:], block[:pairs]], axis=0)

    first = by_core(chip, 4, 2)
    second = by_core(chip, 1, 6)
    crossed = exchange(jnp.concatenate([first, second], axis=0), C, 1)
    third, fourth = turned(crossed[: 2 * pairs]), turned(crossed[2 * pairs :])
    odd_core = lax.axis_index(C) == 1
    six, beside_one = jnp.where(odd_core, second, fourth), jnp.where(odd_core, fourth, second)
    even = jnp.concatenate([first, third, six], axis=0)
    far = exchange(even, Z, 1)
    far, log_scale, logit_bias = lax.optimization_barrier((far, log_scale, logit_bias))
    lane = lax.broadcasted_iota(jnp.int32, (1, LANES), 1)
    knobs = jnp.where(lane == 0, log_scale[0], logit_bias[0])

    rows, unit_text, text_norm = local(
        text_rows, [VMEM] * 6,
        ((plane, pairs, wide), BF16), ((pairs, width), F32), ((pairs, 1), F32),
    )(tile, sides, pooled, arrived, other, gain)
    texts = to_all(rows, PLANE).reshape(plane * pairs, wide)

    text_part, keep, send = local(
        pair_math, [VMEM] * 7,
        ((plane * pairs, wide + LANES), BF16), ((depth * pairs, width), F32), ((depth * pairs, width), BF16),
        to=[HBM, VMEM, VMEM],
        scratch=(
            pltpu.VMEM((plane * pairs, width), BF16), pltpu.VMEM((plane * pairs, 2 * LANES), BF16),
            pltpu.SemaphoreType.DMA((2,)),
        ),
    )(knobs, chip, even, beside_one, far, texts, gain)

    back = to_all(text_part.reshape(plane, pairs, wide + LANES), PLANE)
    came = exchange(send, C, 1)
    pooled_grad, last, totals = local(
        text_gradient, [VMEM, VMEM, VMEM, VMEM],
        ((pairs, width), F32), ((1, width), F32), ((pairs, 2 * LANES), F32),
    )(back, unit_text, text_norm, gain)
    other = exchange(totals, C, 1)
    (blocks,) = local(pack, [SMEM] + [VMEM] * 4, ((depth, pairs, width + 2 * LANES), BF16))(
        lax.axis_index((Z, C))[None], keep, came, totals, other
    )
    line_back = to_all(blocks, Z)
    behind_chip = beside(last, False)
    behind_core = exchange(last, C, 1)
    (token_grad,) = local(token_rows, [VMEM] * 5, ((tokens, width), F32))(ids, sides, pooled_grad, behind_chip, behind_core)
    image_grad, gain_grad, scalars = local(
        functools.partial(finish, count=float(total_pairs * total_pairs)), [VMEM] * 3,
        ((pairs, width), F32), ((width,), F32), ((3,), F32),
    )(line_back, unit_image, image_norm)
    return (image_grad, token_grad, gain_grad, scalars)


def solution(mesh):
    finer = Mesh(mesh.devices.reshape(4, 4, 8, 2), DP)
    placed = (P(DP, None), P(DP, None), P(DP), P(DP), P(), P(), P())
    return jax.shard_map(
        per_device,
        mesh=finer,
        in_specs=placed,
        out_specs=(P(DP, None), P(DP, None), P(), P()),
        check_vma=False,
    )
```
